64 devices in a mesh: dp: 4 (over x, y), x: 16 (over z, core).
Axes of the slice: x: 2, y: 2, z: 8, core: 2. Of those that a mesh axis runs over, the one named last changes fastest.
The devices are a block of a 4x4x8 slice.
Arguments:
- c_raw: bfloat16 [512, 1024, 512], P('dp', 'x'), parts along dimension 0
- k_raw: bfloat16 [512, 1024, 64], P('dp', 'x'), parts along dimension 0
- norm_gain: bfloat16 [512], replicated
- rope_cos: float32 [1024, 32], P('x')
- rope_sin: float32 [1024, 32], P('x')
- seq_lens: int32 [512], P('dp'), parts along dimension 0
- q_lat: bfloat16 [512, 128, 512], P(('dp', 'x')), parts along dimension 0
- q_rope: bfloat16 [512, 128, 64], P(('dp', 'x')), parts along dimension 0
Outputs:
- output 1: bfloat16 [512, 1024, 512], P(('dp', 'x')), parts along dimension 0
- output 2: bfloat16 [512, 1024, 64], P(('dp', 'x')), parts along dimension 0
- output 3: bfloat16 [512, 128, 512], P(('dp', 'x')), parts along dimension 0
There are 4 independent parts. The reference program is written for one: setup_inputs(seed, part) draws one part's arguments, and reference() takes and returns one part's arrays. A program takes and returns all parts, laid end to end along the dimension named above; an argument that names none is the same for every part.
All inputs are finite; a program needn't handle non-finite values.
Results may differ from the reference program's by a relative error of at most 0.00587817.
Values are sent between devices in bfloat16 or wider.
A program may use at most 768 MiB of HBM per device.

```python
import jax
import jax.numpy as jnp
from jax import lax

REQUESTS = 128
SEQ_LEN = 1024
KV_RANK = 512
ROPE_DIM = 64
NUM_HEADS = 128

NORM_EPS = 1e-6
ATTN_SCALE = (KV_RANK + ROPE_DIM) ** -0.5


def setup_inputs(seed: int = 0, part: int = 0) -> dict:
    part_key = jax.random.fold_in(jax.random.key(seed), part)
    keys = jax.random.split(part_key, 8)
    shared = jax.random.split(jax.random.key(seed + 1), 2)
    row_scale = jnp.exp(0.5 * jax.random.normal(keys[0], (REQUESTS, SEQ_LEN, 1), jnp.float32))
    c_raw = (jax.random.normal(keys[1], (REQUESTS, SEQ_LEN, KV_RANK), jnp.float32) * row_scale).astype(jnp.bfloat16)
    k_raw = jax.random.normal(keys[2], (REQUESTS, SEQ_LEN, ROPE_DIM), jnp.float32).astype(jnp.bfloat16)
    norm_gain = (1.0 + 0.3 * jax.random.normal(shared[0], (KV_RANK,), jnp.float32)).astype(jnp.bfloat16)
    half_dim = ROPE_DIM // 2
    log_base = jax.random.uniform(shared[1], (), jnp.float32, 9.0, 14.0)
    inv_freq = jnp.exp(-log_base * (2.0 * jnp.arange(half_dim, dtype=jnp.float32) / ROPE_DIM))
    angles = jnp.arange(SEQ_LEN, dtype=jnp.float32)[:, None] * inv_freq[None, :]
    seq_lens = jax.random.randint(keys[3], (REQUESTS,), SEQ_LEN // 8, SEQ_LEN + 1)
    full_index = jax.random.randint(keys[4], (), 0, REQUESTS)
    short_offset = jax.random.randint(keys[5], (), 1, REQUESTS)
    seq_lens = seq_lens.at[full_index].set(SEQ_LEN)
    seq_lens = seq_lens.at[(full_index + short_offset) % REQUESTS].set(SEQ_LEN // 8)
    q_lat = (1.3 * jax.random.normal(keys[6], (REQUESTS, NUM_HEADS, KV_RANK), jnp.float32)).astype(jnp.bfloat16)
    q_rope = (3.0 * jax.random.normal(keys[7], (REQUESTS, NUM_HEADS, ROPE_DIM), jnp.float32)).astype(jnp.bfloat16)
    return {"c_raw": c_raw, "k_raw": k_raw, "norm_gain": norm_gain, "rope_cos": jnp.cos(angles), "rope_sin": jnp.sin(angles), "seq_lens": seq_lens.astype(jnp.int32), "q_lat": q_lat, "q_rope": q_rope}


def reference(c_raw, k_raw, norm_gain, rope_cos, rope_sin, seq_lens, q_lat, q_rope):
    positions = jnp.arange(SEQ_LEN)
    half_dim = ROPE_DIM // 2
    gain = norm_gain.astype(jnp.float32)

    def one_request(operands):
        c_row, k_row, length, lat_row, rope_row = operands
        valid = positions < length
        lat_f32 = c_row.astype(jnp.float32)
        inv_rms = lax.rsqrt(jnp.mean(lat_f32 * lat_f32, axis=-1, keepdims=True) + NORM_EPS)
        c_norm = jnp.where(valid[:, None], lat_f32 * inv_rms * gain, 0.0).astype(jnp.bfloat16)
        key_f32 = k_row.astype(jnp.float32)
        key_lo = key_f32[:, :half_dim]
        key_hi = key_f32[:, half_dim:]
        rotated = jnp.concatenate([key_lo * rope_cos - key_hi * rope_sin, key_hi * rope_cos + key_lo * rope_sin], axis=-1)
        k_rope = jnp.where(valid[:, None], rotated, 0.0).astype(jnp.bfloat16)
        scores = jnp.dot(lat_row, c_norm.T, preferred_element_type=jnp.float32) + jnp.dot(rope_row, k_rope.T, preferred_element_type=jnp.float32)
        scores = jnp.where(valid[None, :], scores * ATTN_SCALE, -1e30)
        weights = jnp.exp(scores - jnp.max(scores, axis=-1, keepdims=True))
        out_row = jnp.dot(weights, c_norm.astype(jnp.float32)) / jnp.sum(weights, axis=-1, keepdims=True)
        return c_norm, k_rope, out_row.astype(jnp.bfloat16)

    c_cache, kr_cache, o_lat = lax.map(one_request, (c_raw, k_raw, seq_lens, q_lat, q_rope))
    return (c_cache, kr_cache, o_lat)
```

```python
import functools

import jax
import jax.numpy as jnp
from jax import lax
from jax.experimental import pallas as pl
from jax.experimental.pallas import tpu as pltpu
from jax.sharding import PartitionSpec as P

NORM_EPS = 1e-6
MESH = pl.DeviceIdType.MESH
LOOKAHEAD = 2


def partner_order(n):
    chips = n // 2
    order = [(0, 1)]
    for dist in range(1, chips // 2 + 1):
        for core in (0, 1):
            order.append((dist, core))
            if 2 * dist != chips:
                order.append((-dist, core))
    return order


def exchange_kernel(n, lens_ref, lens_row_ref, gain_ref, cos_ref, sin_ref, c_hbm, k_hbm, ql_hbm, qr_hbm, recv, kr_out, o_ref, send, k_raw, rot, turned, kr_send, kr_recv, q_lat, q_rope, load_sem, send_sem, recv_sem, kr_send_sem, kr_recv_sem):
    me = lax.axis_index("x")
    chips = n // 2
    my_chip, my_core = me // 2, lax.rem(me, 2)
    slots, _, seq_local, rank = send.shape
    half = cos_ref.shape[0]
    seq_len = recv.shape[1]
    attn_scale = (rank + 2 * half) ** -0.5
    partners = [2 * lax.rem(my_chip + dist + chips, chips) + lax.rem(my_core + core, 2) for dist, core in partner_order(n)]

    barrier = pltpu.get_barrier_semaphore()
    for target in partners:
        pl.semaphore_signal(barrier, inc=1, device_id={"x": target}, device_id_type=MESH)

    def load_c(slot):
        return pltpu.make_async_copy(c_hbm.at[:, slot], send.at[slot], load_sem.at[slot])

    load_k = pltpu.make_async_copy(k_hbm, k_raw, load_sem.at[slots])
    load_ql = pltpu.make_async_copy(ql_hbm, q_lat, load_sem.at[slots + 1])
    load_qr = pltpu.make_async_copy(qr_hbm, q_rope, load_sem.at[slots + 2])
    load_c(0).start()

    gain = gain_ref[...].astype(jnp.float32)
    row_pos = me * seq_local + lax.broadcasted_iota(jnp.int32, (seq_local, 1), 0)

    def norm_slot(slot):
        def one(dest, carry):
            rows = send[slot, dest].astype(jnp.float32)
            inv_rms = lax.rsqrt(jnp.mean(rows * rows, axis=-1, keepdims=True) + NORM_EPS)
            valid = row_pos < lens_ref[dest * slots + slot]
            normed = jnp.where(valid, rows * inv_rms * gain, 0.0).astype(jnp.bfloat16)
            send[slot, dest] = normed

            @pl.when(dest == me)
            def _():
                recv[slot, pl.ds(pl.multiple_of(me * seq_local, seq_local), seq_local)] = normed

            return carry

        lax.fori_loop(0, n, one, 0)

    def c_copy(slot, i):
        return pltpu.make_async_remote_copy(
            src_ref=send.at[slot, partners[i]],
            dst_ref=recv.at[slot, pl.ds(pl.multiple_of(me * seq_local, seq_local), seq_local)],
            send_sem=send_sem.at[slot, i],
            recv_sem=recv_sem.at[slot, i],
            device_id={"x": partners[i]},
            device_id_type=MESH,
        )

    def kr_copy(i):
        return pltpu.make_async_remote_copy(
            src_ref=kr_send.at[partners[i]],
            dst_ref=kr_recv.at[me],
            send_sem=kr_send_sem.at[i],
            recv_sem=kr_recv_sem.at[i],
            device_id={"x": partners[i]},
            device_id_type=MESH,
        )

    load_c(0).wait()
    load_k.start()
    for slot in range(1, slots):
        load_c(slot).start()
    load_ql.start()
    load_qr.start()
    norm_slot(0)
    pl.semaphore_wait(barrier, n - 1)
    for i in range(n - 1):
        c_copy(0, i).start()

    load_k.wait()
    lens_row = lens_row_ref[...]
    for pos in range(seq_local):
        lo = k_raw[pos, :half, :].astype(jnp.float32)
        hi = k_raw[pos, half:, :].astype(jnp.float32)
        cos = cos_ref[:, pos : pos + 1]
        sin = sin_ref[:, pos : pos + 1]
        valid = me * seq_local + pos < lens_row
        rot[2 * half * pos : 2 * half * pos + half, :] = jnp.where(valid, lo * cos - hi * sin, 0.0)
        rot[2 * half * pos + half : 2 * half * (pos + 1), :] = jnp.where(valid, hi * cos + lo * sin, 0.0)
    requests = n * slots
    for dim in range(half):
        lo = rot[pl.ds(dim, seq_local, stride=2 * half), :]
        hi = rot[pl.ds(half + dim, seq_local, stride=2 * half), :]
        turned[pl.ds(dim, requests, stride=half), :] = jnp.concatenate([lo, hi], axis=0).T
    for dest in range(n):
        kr_send[dest] = turned[dest * slots * half : (dest + 1) * slots * half, :].astype(jnp.bfloat16)
    kr_recv[me] = kr_send[me]

    for slot in range(1, LOOKAHEAD):
        load_c(slot).wait()
        norm_slot(slot)
    for i in range(n - 1):
        kr_copy(i).start()
    for slot in range(1, LOOKAHEAD):
        for i in range(n - 1):
            c_copy(slot, i).start()
    load_ql.wait()
    load_qr.wait()
    low_lanes = lax.broadcasted_iota(jnp.int32, (half, 2 * seq_local), 1) < seq_local
    key_pos = lax.broadcasted_iota(jnp.int32, (1, seq_len), 1)

    def one_slot(slot, carry):
        @pl.when(slot + LOOKAHEAD < slots)
        def _():
            ahead = slot + LOOKAHEAD
            load_c(ahead).wait()
            norm_slot(ahead)
            for i in range(n - 1):
                c_copy(ahead, i).start()

        @pl.when(slot == 0)
        def _():
            for i in range(n - 1):
                kr_copy(i).wait_recv()

        for pair in range(chips):
            even = kr_recv[2 * pair, pl.ds(pl.multiple_of(slot * half, half), half), :].astype(jnp.float32)
            odd = kr_recv[2 * pair + 1, pl.ds(pl.multiple_of(slot * half, half), half), :].astype(jnp.float32)
            lanes = slice(2 * seq_local * pair, 2 * seq_local * (pair + 1))
            kr_out[slot, :half, lanes] = jnp.where(low_lanes, even, pltpu.roll(odd, seq_local, 1)).astype(jnp.bfloat16)
            kr_out[slot, half:, lanes] = jnp.where(low_lanes, pltpu.roll(even, seq_local, 1), odd).astype(jnp.bfloat16)
        rope_q = q_rope[slot].astype(jnp.float32).T.astype(jnp.bfloat16)
        scores = jnp.dot(rope_q, kr_out[slot], preferred_element_type=jnp.float32)

        for i in range(n - 1):
            c_copy(slot, i).wait_recv()
        cache = recv[slot]
        scores += lax.dot_general(q_lat[slot], cache, (((1,), (1,)), ((), ())), preferred_element_type=jnp.float32)
        valid = key_pos < lens_ref[me * slots + slot]
        scores = jnp.where(valid, scores * attn_scale, -1e30)
        weights = jnp.exp(scores - jnp.max(scores, axis=-1, keepdims=True))
        weight_sum = jnp.sum(weights, axis=-1, keepdims=True)
        weighted = jnp.dot(weights.astype(jnp.bfloat16), cache, preferred_element_type=jnp.float32)
        o_ref[slot] = (weighted / weight_sum).astype(jnp.bfloat16)
        return carry

    lax.fori_loop(0, slots, one_slot, 0)
    for i in range(n - 1):
        kr_copy(i).wait_send()

    def drain(slot, carry):
        for i in range(n - 1):
            c_copy(slot, i).wait_send()
        return carry

    lax.fori_loop(0, slots, drain, 0)


def store_kernel(c_ref, kr_ref, o_ref, c_out, kr_out, o_out, sem):
    copies = [pltpu.make_async_copy(src, dst, sem.at[i]) for i, (src, dst) in enumerate([(c_ref, c_out), (kr_ref, kr_out), (o_ref, o_out)])]
    for copy in copies:
        copy.start()
    for copy in copies:
        copy.wait()


def solution(mesh):
    n = mesh.shape["x"]
    seq_spec = P("dp", "x", None)
    req_spec = P(("dp", "x"), None, None)

    def local_step(c_raw, k_raw, norm_gain, rope_cos, rope_sin, seq_lens, q_lat, q_rope):
        requests, seq_local, rank = c_raw.shape
        slots, heads, _ = q_lat.shape
        rope_dim = k_raw.shape[-1]
        half = rope_dim // 2
        seq_len = n * seq_local
        bf16, f32 = jnp.bfloat16, jnp.float32
        hbm = pl.BlockSpec(memory_space=pltpu.HBM)
        vmem = pl.BlockSpec(memory_space=pltpu.VMEM)
        smem = pl.BlockSpec(memory_space=pltpu.SMEM)
        outs = [((slots, seq_len, rank), bf16), ((slots, rope_dim, seq_len), bf16), ((slots, heads, rank), bf16)]
        c_got, kr_got, o_got = pl.pallas_call(
            functools.partial(exchange_kernel, n),
            out_shape=[pltpu.VMEM(*out) for out in outs],
            in_specs=[smem, vmem, vmem, vmem, vmem, hbm, hbm, hbm, hbm],
            out_specs=[vmem] * 3,
            scratch_shapes=[
                pltpu.VMEM((slots, n, seq_local, rank), bf16),
                pltpu.VMEM((seq_local, rope_dim, requests), bf16),
                pltpu.VMEM((seq_local * rope_dim, requests), f32),
                pltpu.VMEM((requests * half, 2 * seq_local), f32),
                pltpu.VMEM((n, slots * half, 2 * seq_local), bf16),
                pltpu.VMEM((n, slots * half, 2 * seq_local), bf16),
                pltpu.VMEM(q_lat.shape, bf16),
                pltpu.VMEM((slots, rope_dim, heads), bf16),
                pltpu.SemaphoreType.DMA((slots + 3,)),
                pltpu.SemaphoreType.DMA((slots, n - 1)),
                pltpu.SemaphoreType.DMA((slots, n - 1)),
                pltpu.SemaphoreType.DMA((n - 1,)),
                pltpu.SemaphoreType.DMA((n - 1,)),
            ],
            compiler_params=pltpu.CompilerParams(collective_id=0, has_side_effects=True, vmem_limit_bytes=40 * 1024 * 1024),
            name="exchange",
        )(
            seq_lens,
            seq_lens.reshape(1, requests),
            norm_gain.reshape(1, rank),
            rope_cos.T,
            rope_sin.T,
            c_raw.reshape(n, slots, seq_local, rank),
            jnp.transpose(k_raw, (1, 2, 0)),
            q_lat,
            jnp.transpose(q_rope, (0, 2, 1)),
        )
        c_cache, kr_cache, o_lat = pl.pallas_call(
            store_kernel,
            out_shape=[jax.ShapeDtypeStruct(*out) for out in outs],
            in_specs=[vmem] * 3,
            out_specs=[hbm] * 3,
            scratch_shapes=[pltpu.SemaphoreType.DMA((3,))],
            compiler_params=pltpu.CompilerParams(vmem_limit_bytes=8 * 1024 * 1024),
            name="store",
        )(c_got, kr_got, o_got)
        return c_cache, jnp.transpose(kr_cache, (0, 2, 1)), o_lat

    return jax.shard_map(local_step, mesh=mesh, in_specs=(seq_spec, seq_spec, P(None), P("x", None), P("x", None), P("dp"), req_spec, req_spec), out_specs=(req_spec, req_spec, req_spec), check_vma=False)
```

```python
import functools

import jax
import jax.numpy as jnp
from jax import lax
from jax.experimental import pallas as pl
from jax.experimental.pallas import tpu as pltpu
from jax.sharding import PartitionSpec as P

NORM_EPS = 1e-6
MASKED = -3.0e38
MESH = pl.DeviceIdType.MESH


def message_order(chips, slots):
    order = []
    for dist in range(1, chips // 2):
        for core in (0, 1):
            for sign in (1, -1):
                order.append((sign * dist, core, 0, slots))
    order.insert(4, (0, 1, 0, slots))
    for first in (0, slots // 2):
        for core in (0, 1):
            order.append((chips // 2, core, first, slots // 2))
    return order


def attend_chunk(r, chip, q_lat, rope_q, recv, kr_out, acc, top, total, own_lens, attn_scale):
    width = own_lens.shape[-1]
    start = pl.multiple_of(chip * width, width)
    rows = recv[r, pl.ds(start, width), :]
    keys = kr_out[r, :, pl.ds(start, width)]
    scores = lax.dot_general(q_lat[r], rows, (((1,), (1,)), ((), ())), preferred_element_type=jnp.float32)
    scores += jnp.dot(rope_q[r], keys, preferred_element_type=jnp.float32)
    pos = start + lax.broadcasted_iota(jnp.int32, (1, width), 1)
    valid = pos < own_lens[r]
    scores = jnp.where(valid, scores * attn_scale, MASKED)
    old_top = top[r]
    new_top = jnp.maximum(old_top, jnp.max(scores, axis=-1, keepdims=True))
    weights = jnp.where(valid, jnp.exp(scores - new_top), 0.0)
    decay = jnp.exp(old_top - new_top)
    top[r] = new_top
    new_total = total[r] * decay + jnp.sum(weights, axis=-1, keepdims=True)
    total[r] = new_total
    mixed = acc[r] * decay + jnp.dot(weights.astype(jnp.bfloat16), rows, preferred_element_type=jnp.float32)
    return mixed, new_total


def exchange_kernel(n, lens_hbm, lens_row_hbm, gain_hbm, cos_hbm, sin_hbm, c_hbm, k_hbm, ql_hbm, qr_hbm, recv, kr_out, acc, top, total, q_lat, rope_q, own_lens, lens, lens_row, gain_ref, cos_ref, sin_ref, send, k_raw, rot, turned, kr_send, kr_recv, q_rope, small_sem, load_sem, send_sem, recv_sem, kr_send_sem, kr_recv_sem):
    me = lax.axis_index("x")
    chips = n // 2
    my_chip, my_core = me // 2, lax.rem(me, 2)
    _, slots, seq_local, rank = send.shape
    half = cos_ref.shape[0]
    attn_scale = (rank + 2 * half) ** -0.5
    messages = message_order(chips, slots)

    def device(dist, core):
        return 2 * lax.rem(my_chip + dist + chips, chips) + lax.rem(my_core + core, 2)

    partners = []
    for dist, core, _, _ in messages:
        if (dist, core) not in partners:
            partners.append((dist, core))
    targets = [device(*partner) for partner in partners]

    barrier = pltpu.get_barrier_semaphore()
    for target in targets:
        pl.semaphore_signal(barrier, inc=1, device_id={"x": target}, device_id_type=MESH)

    def load_c(i):
        dest = me if i == n - 1 else targets[i]
        return pltpu.make_async_copy(c_hbm.at[dest], send.at[dest], load_sem.at[i])

    small = [(lens_hbm, lens), (gain_hbm, gain_ref), (lens_row_hbm, lens_row), (cos_hbm, cos_ref), (sin_hbm, sin_ref), (k_hbm, k_raw), (qr_hbm, q_rope), (ql_hbm, q_lat)]
    small = [pltpu.make_async_copy(src, dst, small_sem.at[i]) for i, (src, dst) in enumerate(small)]
    for copy in small[:2]:
        copy.start()
    for i in range(4):
        load_c(i).start()
    for copy in small[2:]:
        copy.start()
    for i in range(4, n):
        load_c(i).start()
    for copy in small[:2]:
        copy.wait()

    gain = gain_ref[...].astype(jnp.float32).reshape(1, rank)
    row_pos = me * seq_local + lax.broadcasted_iota(jnp.int32, (seq_local, 1), 0)

    def norm_rows(i):
        load_c(i).wait()
        dest = me if i == n - 1 else targets[i]

        def one(slot, carry):
            rows = send[dest, slot].astype(jnp.float32)
            inv_rms = lax.rsqrt(jnp.mean(rows * rows, axis=-1, keepdims=True) + NORM_EPS)
            valid = row_pos < lens[dest * slots + slot]
            normed = jnp.where(valid, rows * inv_rms * gain, 0.0).astype(jnp.bfloat16)
            if i == n - 1:
                recv[slot, pl.ds(pl.multiple_of(me * seq_local, seq_local), seq_local), :] = normed
            else:
                send[dest, slot] = normed
            return carry

        lax.fori_loop(0, slots, one, 0, unroll=2)

    def c_copy(m):
        dist, core, first, count = messages[m]
        target = device(dist, core)
        return pltpu.make_async_remote_copy(
            src_ref=send.at[target, pl.ds(first, count)],
            dst_ref=recv.at[pl.ds(first, count), pl.ds(pl.multiple_of(me * seq_local, seq_local), seq_local)],
            send_sem=send_sem.at[m],
            recv_sem=recv_sem.at[m],
            device_id={"x": target},
            device_id_type=MESH,
        )

    def kr_copy(i):
        return pltpu.make_async_remote_copy(
            src_ref=kr_send.at[targets[i]],
            dst_ref=kr_recv.at[me],
            send_sem=kr_send_sem.at[i],
            recv_sem=kr_recv_sem.at[i],
            device_id={"x": targets[i]},
            device_id_type=MESH,
        )

    def send_rows(i):
        for m, (dist, core, _, _) in enumerate(messages):
            if (dist, core) == partners[i]:
                c_copy(m).start()

    early = 5
    norm_rows(0)
    norm_rows(1)
    pl.semaphore_wait(barrier, n - 1)
    for i in range(2, early):
        send_rows(i - 2)
        norm_rows(i)
    send_rows(early - 2)
    send_rows(early - 1)

    for copy in small[2:]:
        copy.wait()
    lens_vec = lens_row[...]
    for pos in range(seq_local):
        lo = k_raw[pos, :half, :].astype(jnp.float32)
        hi = k_raw[pos, half:, :].astype(jnp.float32)
        cos = cos_ref[:, pos : pos + 1]
        sin = sin_ref[:, pos : pos + 1]
        valid = me * seq_local + pos < lens_vec
        rot[2 * half * pos : 2 * half * pos + half, :] = jnp.where(valid, lo * cos - hi * sin, 0.0)
        rot[2 * half * pos + half : 2 * half * (pos + 1), :] = jnp.where(valid, hi * cos + lo * sin, 0.0)
    requests = n * slots
    for dim in range(half):
        lo = rot[pl.ds(dim, seq_local, stride=2 * half), :]
        hi = rot[pl.ds(half + dim, seq_local, stride=2 * half), :]
        turned[pl.ds(dim, requests, stride=half), :] = jnp.concatenate([lo, hi], axis=0).T
    for dest in range(n):
        kr_send[dest] = turned[dest * slots * half : (dest + 1) * slots * half, :].astype(jnp.bfloat16)
    kr_recv[me] = kr_send[me]

    norm_rows(early)
    for i in range(n - 1):
        kr_copy(i).start()
    for i in range(early + 1, n - 1):
        send_rows(i - 1)
        norm_rows(i)
    send_rows(n - 2)
    norm_rows(n - 1)

    for slot in range(slots):
        rope_q[slot] = q_rope[slot].astype(jnp.float32).T.astype(jnp.bfloat16)
        own_lens[slot] = jnp.full(own_lens.shape[1:], lens[me * slots + slot], jnp.int32)
    acc[...] = jnp.zeros_like(acc)
    top[...] = jnp.full_like(top, MASKED)
    total[...] = jnp.zeros_like(total)

    low_lanes = lax.broadcasted_iota(jnp.int32, (half, 2 * seq_local), 1) < seq_local

    def gather_chip(dist):
        chip = lax.rem(my_chip + dist + chips, chips)
        for i, (far, _) in enumerate(partners):
            if (far + dist) % chips == 0:
                kr_copy(i).wait_recv()
        start = pl.multiple_of(chip * 2 * seq_local, 2 * seq_local)
        for slot in range(slots):
            even = kr_recv[2 * chip, slot * half : (slot + 1) * half, :].astype(jnp.float32)
            odd = kr_recv[2 * chip + 1, slot * half : (slot + 1) * half, :].astype(jnp.float32)
            kr_out[slot, :half, pl.ds(start, 2 * seq_local)] = jnp.where(low_lanes, even, pltpu.roll(odd, seq_local, 1)).astype(jnp.bfloat16)
            kr_out[slot, half:, pl.ds(start, 2 * seq_local)] = jnp.where(low_lanes, pltpu.roll(even, seq_local, 1), odd).astype(jnp.bfloat16)
        for m, (far, _, _, _) in enumerate(messages):
            if (far + dist) % chips == 0:
                c_copy(m).wait_recv()
        return chip

    for dist in [0] + [sign * far for far in range(1, chips // 2) for sign in (1, -1)]:
        chip = gather_chip(dist)

        def one_request(r, carry, chip=chip):
            acc[r], _ = attend_chunk(r, chip, q_lat, rope_q, recv, kr_out, acc, top, total, own_lens, attn_scale)
            return carry

        lax.fori_loop(0, slots, one_request, 0, unroll=2)

    for i in range(n - 1):
        kr_copy(i).wait_send()
    gather_chip(chips // 2)
    for m in range(len(messages)):
        c_copy(m).wait_send()


def finish_kernel(n, attn_scale, recv, kr_in, acc, top_in, total_in, q_lat, rope_q, own_lens, c_out, kr_out, o_out, top, total, o_ref, sem):
    chips = n // 2
    slots = acc.shape[0]
    copies = [pltpu.make_async_copy(recv.at[r], c_out.at[r], sem.at[r]) for r in range(slots)]
    copies.append(pltpu.make_async_copy(kr_in, kr_out, sem.at[slots]))
    for copy in copies:
        copy.start()
    top[...] = top_in[...]
    total[...] = total_in[...]
    chip = lax.rem(lax.axis_index("x") // 2 + chips // 2, chips)
    for r in range(slots):
        mixed, weight_sum = attend_chunk(r, chip, q_lat, rope_q, recv, kr_in, acc, top, total, own_lens, attn_scale)
        o_ref[r] = (mixed / weight_sum).astype(jnp.bfloat16)
        copies.append(pltpu.make_async_copy(o_ref.at[r], o_out.at[r], sem.at[slots + 1 + r]))
        copies[-1].start()
    for copy in copies:
        copy.wait()


def solution(mesh):
    n = mesh.shape["x"]
    seq_spec = P("dp", "x", None)
    req_spec = P(("dp", "x"), None, None)

    def local_step(c_raw, k_raw, norm_gain, rope_cos, rope_sin, seq_lens, q_lat, q_rope):
        requests, seq_local, rank = c_raw.shape
        slots, heads, _ = q_lat.shape
        rope_dim = k_raw.shape[-1]
        half = rope_dim // 2
        seq_len = n * seq_local
        bf16, f32, i32 = jnp.bfloat16, jnp.float32, jnp.int32
        hbm = pl.BlockSpec(memory_space=pltpu.HBM)
        vmem = pl.BlockSpec(memory_space=pltpu.VMEM)
        messages = len(message_order(n // 2, slots))
        passed = [
            ((slots, seq_len, rank), bf16),
            ((slots, rope_dim, seq_len), bf16),
            ((slots, heads, rank), f32),
            ((slots, heads, 1), f32),
            ((slots, heads, 1), f32),
            ((slots, heads, rank), bf16),
            ((slots, heads, rope_dim), bf16),
            ((slots, 1, 2 * seq_local), i32),
        ]
        operands = (
            seq_lens,
            seq_lens.reshape(1, requests),
            norm_gain,
            rope_cos.T,
            rope_sin.T,
            c_raw.reshape(n, slots, seq_local, rank),
            jnp.transpose(k_raw, (1, 2, 0)),
            q_lat,
            jnp.transpose(q_rope, (0, 2, 1)),
        )
        got = pl.pallas_call(
            functools.partial(exchange_kernel, n),
            out_shape=[pltpu.VMEM(*out) for out in passed],
            in_specs=[hbm] * len(operands),
            out_specs=[vmem] * len(passed),
            scratch_shapes=[
                pltpu.SMEM((requests,), i32),
                pltpu.VMEM((1, requests), i32),
                pltpu.VMEM((rank,), bf16),
                pltpu.VMEM((half, seq_local), f32),
                pltpu.VMEM((half, seq_local), f32),
                pltpu.VMEM((n, slots, seq_local, rank), bf16),
                pltpu.VMEM((seq_local, rope_dim, requests), bf16),
                pltpu.VMEM((seq_local * rope_dim, requests), f32),
                pltpu.VMEM((requests * half, 2 * seq_local), f32),
                pltpu.VMEM((n, slots * half, 2 * seq_local), bf16),
                pltpu.VMEM((n, slots * half, 2 * seq_local), bf16),
                pltpu.VMEM((slots, rope_dim, heads), bf16),
                pltpu.SemaphoreType.DMA((8,)),
                pltpu.SemaphoreType.DMA((n,)),
                pltpu.SemaphoreType.DMA((messages,)),
                pltpu.SemaphoreType.DMA((messages,)),
                pltpu.SemaphoreType.DMA((n - 1,)),
                pltpu.SemaphoreType.DMA((n - 1,)),
            ],
            compiler_params=pltpu.CompilerParams(collective_id=0, has_side_effects=True, vmem_limit_bytes=40 * 1024 * 1024),
            name="exchange",
        )(*[pltpu.with_memory_space_constraint(x, pltpu.HBM) for x in operands])
        outs = [((slots, seq_len, rank), bf16), ((slots, rope_dim, seq_len), bf16), ((slots, heads, rank), bf16)]
        c_cache, kr_cache, o_lat = pl.pallas_call(
            functools.partial(finish_kernel, n, (rank + rope_dim) ** -0.5),
            out_shape=[jax.ShapeDtypeStruct(*out) for out in outs],
            in_specs=[vmem] * len(passed),
            out_specs=[hbm] * 3,
            scratch_shapes=[
                pltpu.VMEM((slots, heads, 1), f32),
                pltpu.VMEM((slots, heads, 1), f32),
                pltpu.VMEM((slots, heads, rank), bf16),
                pltpu.SemaphoreType.DMA((2 * slots + 1,)),
            ],
            compiler_params=pltpu.CompilerParams(vmem_limit_bytes=8 * 1024 * 1024),
            name="finish",
        )(*got)
        return c_cache, jnp.transpose(kr_cache, (0, 2, 1)), o_lat

    return jax.shard_map(local_step, mesh=mesh, in_specs=(seq_spec, seq_spec, P(None), P("x", None), P("x", None), P("dp"), req_spec, req_spec), out_specs=(req_spec, req_spec, req_spec), check_vma=False)
```

```python
import functools

import jax
import jax.numpy as jnp
from jax import lax
from jax.experimental import pallas as pl
from jax.experimental.pallas import tpu as pltpu
from jax.sharding import PartitionSpec as P

NORM_EPS = 1e-6
MASKED = -3.0e38
MESH = pl.DeviceIdType.MESH
DISTANCES = (1, 3, 2)
RAW = 2


def message_order(chips, slots):
    far = chips // 2
    order = []
    for dist in DISTANCES:
        for core in (0, 1):
            for sign in (1, -1):
                order.append((sign * dist, core, 0, slots))
    order.insert(4, (0, 1, 0, slots))
    for first in (0, slots // 2):
        for core in (0, 1):
            order.append((far, core, first, slots // 2))
    return order


def normed_rows(rows, gain, first_pos, length):
    rows = rows.astype(jnp.float32)
    inv_rms = lax.rsqrt(jnp.mean(rows * rows, axis=-1, keepdims=True) + NORM_EPS)
    valid = first_pos + lax.broadcasted_iota(jnp.int32, (rows.shape[0], 1), 0) < length
    return jnp.where(valid, rows * inv_rms * gain, 0.0).astype(jnp.bfloat16)


def attend_chunk(r, chip, q_lat, rope_q, recv, kr_out, acc, top, total, own_lens, attn_scale):
    width = own_lens.shape[-1]
    start = pl.multiple_of(chip * width, width)
    rows = recv[r, pl.ds(start, width), :]
    keys = kr_out[r, :, pl.ds(start, width)]
    scores = lax.dot_general(q_lat[r], rows, (((1,), (1,)), ((), ())), preferred_element_type=jnp.float32)
    scores += jnp.dot(rope_q[r], keys, preferred_element_type=jnp.float32)
    pos = start + lax.broadcasted_iota(jnp.int32, (1, width), 1)
    valid = pos < own_lens[r]
    scores = jnp.where(valid, scores * attn_scale, MASKED)
    old_top = top[r]
    new_top = jnp.maximum(old_top, jnp.max(scores, axis=-1, keepdims=True))
    weights = jnp.where(valid, jnp.exp(scores - new_top), 0.0)
    decay = jnp.exp(old_top - new_top)
    top[r] = new_top
    new_total = total[r] * decay + jnp.sum(weights, axis=-1, keepdims=True)
    total[r] = new_total
    mixed = acc[r] * decay + jnp.dot(weights.astype(jnp.bfloat16), rows, preferred_element_type=jnp.float32)
    return mixed, new_total


def exchange_kernel(n, lens_hbm, lens_row_hbm, gain_hbm, cos_hbm, sin_hbm, c_hbm, k_hbm, ql_hbm, qr_hbm, recv, kr_out, acc, top, total, q_lat, rope_q, own_lens, lens, lens_row, gain_ref, cos_ref, sin_ref, send, k_raw, rot, turned, kr_send, kr_recv, q_rope, small_sem, load_sem, send_sem, recv_sem, kr_send_sem, kr_recv_sem, ready):
    me = lax.axis_index("x")
    chips = n // 2
    my_chip, my_core = me // 2, lax.rem(me, 2)
    _, slots, seq_local, rank = send.shape
    half = cos_ref.shape[0]
    attn_scale = (rank + 2 * half) ** -0.5
    messages = message_order(chips, slots)

    def device(dist, core):
        return 2 * lax.rem(my_chip + dist + chips, chips) + lax.rem(my_core + core, 2)

    partners = []
    for dist, core, _, _ in messages:
        if (dist, core) not in partners:
            partners.append((dist, core))
    targets = [device(*partner) for partner in partners]

    near = [device(dist, core) for dist, core in ((1, 0), (-1, 0), (1, 1), (-1, 1), (0, 1))]

    def greet(sem):
        for target in near:
            pl.semaphore_signal(sem, inc=1, device_id={"x": target}, device_id_type=MESH)

    barrier = pltpu.get_barrier_semaphore()
    greet(barrier)

    def load_c(i):
        dest = me if i == n - 1 else targets[i]
        return pltpu.make_async_copy(c_hbm.at[dest], send.at[dest], load_sem.at[i])

    small = [(lens_hbm, lens), (gain_hbm, gain_ref), (lens_row_hbm, lens_row), (cos_hbm, cos_ref), (sin_hbm, sin_ref), (k_hbm, k_raw), (qr_hbm, q_rope), (ql_hbm, q_lat)]
    small = [pltpu.make_async_copy(src, dst, small_sem.at[i]) for i, (src, dst) in enumerate(small)]
    for copy in small[:2]:
        copy.start()
    for i in range(RAW, RAW + 3):
        load_c(i).start()
    for copy in small[2:]:
        copy.start()
    for i in range(RAW + 3, n):
        load_c(i).start()

    def norm_rows(i):
        load_c(i).wait()
        dest = me if i == n - 1 else targets[i]

        def one(slot, carry):
            normed = normed_rows(send[dest, slot], gain, me * seq_local, lens[dest * slots + slot])
            if i == n - 1:
                recv[slot, pl.ds(pl.multiple_of(me * seq_local, seq_local), seq_local), :] = normed
            else:
                send[dest, slot] = normed
            return carry

        lax.fori_loop(0, slots, one, 0, unroll=2)

    def c_copy(m):
        dist, core, first, count = messages[m]
        target = device(dist, core)
        return pltpu.make_async_remote_copy(
            src_ref=(c_hbm if m < RAW else send).at[target, pl.ds(first, count)],
            dst_ref=recv.at[pl.ds(first, count), pl.ds(pl.multiple_of(me * seq_local, seq_local), seq_local)],
            send_sem=send_sem.at[m],
            recv_sem=recv_sem.at[m],
            device_id={"x": target},
            device_id_type=MESH,
        )

    def kr_copy(i):
        return pltpu.make_async_remote_copy(
            src_ref=kr_send.at[targets[i]],
            dst_ref=kr_recv.at[me],
            send_sem=kr_send_sem.at[i],
            recv_sem=kr_recv_sem.at[i],
            device_id={"x": targets[i]},
            device_id_type=MESH,
        )

    def send_rows(i):
        for m, (dist, core, _, _) in enumerate(messages):
            if (dist, core) == partners[i]:
                c_copy(m).start()

    pl.semaphore_wait(barrier, len(near))
    for i in range(RAW):
        send_rows(i)
    greet(ready.at[0])
    for copy in small[:2]:
        copy.wait()
    gain = gain_ref[...].astype(jnp.float32).reshape(1, rank)
    early = 5
    for i in range(RAW, early):
        norm_rows(i)
        send_rows(i)
    for stage in range(chips // 2 - 1):
        pl.semaphore_wait(ready.at[stage], len(near))
        if stage + 1 < chips // 2 - 1:
            greet(ready.at[stage + 1])

    for copy in small[2:]:
        copy.wait()
    lens_vec = lens_row[...]
    for pos in range(seq_local):
        lo = k_raw[pos, :half, :].astype(jnp.float32)
        hi = k_raw[pos, half:, :].astype(jnp.float32)
        cos = cos_ref[:, pos : pos + 1]
        sin = sin_ref[:, pos : pos + 1]
        valid = me * seq_local + pos < lens_vec
        rot[2 * half * pos : 2 * half * pos + half, :] = jnp.where(valid, lo * cos - hi * sin, 0.0)
        rot[2 * half * pos + half : 2 * half * (pos + 1), :] = jnp.where(valid, hi * cos + lo * sin, 0.0)
    requests = n * slots
    for dim in range(half):
        lo = rot[pl.ds(dim, seq_local, stride=2 * half), :]
        hi = rot[pl.ds(half + dim, seq_local, stride=2 * half), :]
        turned[pl.ds(dim, requests, stride=half), :] = jnp.concatenate([lo, hi], axis=0).T
    for dest in range(n):
        kr_send[dest] = turned[dest * slots * half : (dest + 1) * slots * half, :].astype(jnp.bfloat16)
    kr_recv[me] = kr_send[me]

    norm_rows(early)
    for i in range(n - 1):
        kr_copy(i).start()
    for i in range(early + 1, n - 1):
        send_rows(i - 1)
        norm_rows(i)
    send_rows(n - 2)
    norm_rows(n - 1)

    for slot in range(slots):
        rope_q[slot] = q_rope[slot].astype(jnp.float32).T.astype(jnp.bfloat16)
        own_lens[slot] = jnp.full(own_lens.shape[1:], lens[me * slots + slot], jnp.int32)
    acc[...] = jnp.zeros_like(acc)
    top[...] = jnp.full_like(top, MASKED)
    total[...] = jnp.zeros_like(total)

    low_lanes = lax.broadcasted_iota(jnp.int32, (half, 2 * seq_local), 1) < seq_local

    def gather_chip(dist):
        chip = lax.rem(my_chip + dist + chips, chips)
        for i, (far, _) in enumerate(partners):
            if (far + dist) % chips == 0:
                kr_copy(i).wait_recv()
        start = pl.multiple_of(chip * 2 * seq_local, 2 * seq_local)
        for slot in range(slots):
            even = kr_recv[2 * chip, slot * half : (slot + 1) * half, :].astype(jnp.float32)
            odd = kr_recv[2 * chip + 1, slot * half : (slot + 1) * half, :].astype(jnp.float32)
            kr_out[slot, :half, pl.ds(start, 2 * seq_local)] = jnp.where(low_lanes, even, pltpu.roll(odd, seq_local, 1)).astype(jnp.bfloat16)
            kr_out[slot, half:, pl.ds(start, 2 * seq_local)] = jnp.where(low_lanes, pltpu.roll(even, seq_local, 1), odd).astype(jnp.bfloat16)
        for m, (far, _, _, _) in enumerate(messages):
            if (far + dist) % chips == 0:
                c_copy(m).wait_recv()
                if m < RAW:
                    first_pos = pl.multiple_of((2 * chip + lax.rem(my_core + messages[m][1], 2)) * seq_local, seq_local)

                    def one(slot, carry, first_pos=first_pos):
                        recv[slot, pl.ds(first_pos, seq_local), :] = normed_rows(recv[slot, pl.ds(first_pos, seq_local), :], gain, first_pos, lens[me * slots + slot])
                        return carry

                    lax.fori_loop(0, slots, one, 0, unroll=2)
        return chip

    for dist in [0] + [sign * far for far in DISTANCES for sign in (1, -1)]:
        chip = gather_chip(dist)

        def one_request(r, carry, chip=chip):
            acc[r], _ = attend_chunk(r, chip, q_lat, rope_q, recv, kr_out, acc, top, total, own_lens, attn_scale)
            return carry

        lax.fori_loop(0, slots, one_request, 0, unroll=2)

    for i in range(n - 1):
        kr_copy(i).wait_send()
    gather_chip(chips // 2)
    for m in range(len(messages)):
        c_copy(m).wait_send()


def finish_kernel(n, attn_scale, recv, kr_in, acc, top_in, total_in, q_lat, rope_q, own_lens, c_out, kr_out, o_out, top, total, o_ref, sem):
    chips = n // 2
    slots = acc.shape[0]
    copies = [pltpu.make_async_copy(recv.at[r], c_out.at[r], sem.at[r]) for r in range(slots)]
    copies.append(pltpu.make_async_copy(kr_in, kr_out, sem.at[slots]))
    for copy in copies:
        copy.start()
    top[...] = top_in[...]
    total[...] = total_in[...]
    chip = lax.rem(lax.axis_index("x") // 2 + chips // 2, chips)
    for r in range(slots):
        mixed, weight_sum = attend_chunk(r, chip, q_lat, rope_q, recv, kr_in, acc, top, total, own_lens, attn_scale)
        o_ref[r] = (mixed / weight_sum).astype(jnp.bfloat16)
        copies.append(pltpu.make_async_copy(o_ref.at[r], o_out.at[r], sem.at[slots + 1 + r]))
        copies[-1].start()
    for copy in copies:
        copy.wait()


def solution(mesh):
    n = mesh.shape["x"]
    seq_spec = P("dp", "x", None)
    req_spec = P(("dp", "x"), None, None)

    def local_step(c_raw, k_raw, norm_gain, rope_cos, rope_sin, seq_lens, q_lat, q_rope):
        requests, seq_local, rank = c_raw.shape
        slots, heads, _ = q_lat.shape
        rope_dim = k_raw.shape[-1]
        half = rope_dim // 2
        seq_len = n * seq_local
        bf16, f32, i32 = jnp.bfloat16, jnp.float32, jnp.int32
        hbm = pl.BlockSpec(memory_space=pltpu.HBM)
        vmem = pl.BlockSpec(memory_space=pltpu.VMEM)
        messages = len(message_order(n // 2, slots))
        passed = [
            ((slots, seq_len, rank), bf16),
            ((slots, rope_dim, seq_len), bf16),
            ((slots, heads, rank), f32),
            ((slots, heads, 1), f32),
            ((slots, heads, 1), f32),
            ((slots, heads, rank), bf16),
            ((slots, heads, rope_dim), bf16),
            ((slots, 1, 2 * seq_local), i32),
        ]
        operands = (
            seq_lens,
            seq_lens.reshape(1, requests),
            norm_gain,
            rope_cos.T,
            rope_sin.T,
            c_raw.reshape(n, slots, seq_local, rank),
            jnp.transpose(k_raw, (1, 2, 0)),
            q_lat,
            jnp.transpose(q_rope, (0, 2, 1)),
        )
        got = pl.pallas_call(
            functools.partial(exchange_kernel, n),
            out_shape=[pltpu.VMEM(*out) for out in passed],
            in_specs=[hbm] * len(operands),
            out_specs=[vmem] * len(passed),
            scratch_shapes=[
                pltpu.SMEM((requests,), i32),
                pltpu.VMEM((1, requests), i32),
                pltpu.VMEM((rank,), bf16),
                pltpu.VMEM((half, seq_local), f32),
                pltpu.VMEM((half, seq_local), f32),
                pltpu.VMEM((n, slots, seq_local, rank), bf16),
                pltpu.VMEM((seq_local, rope_dim, requests), bf16),
                pltpu.VMEM((seq_local * rope_dim, requests), f32),
                pltpu.VMEM((requests * half, 2 * seq_local), f32),
                pltpu.VMEM((n, slots * half, 2 * seq_local), bf16),
                pltpu.VMEM((n, slots * half, 2 * seq_local), bf16),
                pltpu.VMEM((slots, rope_dim, heads), bf16),
                pltpu.SemaphoreType.DMA((8,)),
                pltpu.SemaphoreType.DMA((n,)),
                pltpu.SemaphoreType.DMA((messages,)),
                pltpu.SemaphoreType.DMA((messages,)),
                pltpu.SemaphoreType.DMA((n - 1,)),
                pltpu.SemaphoreType.DMA((n - 1,)),
                pltpu.SemaphoreType.REGULAR((n // 4 - 1,)),
            ],
            compiler_params=pltpu.CompilerParams(collective_id=0, has_side_effects=True, vmem_limit_bytes=40 * 1024 * 1024),
            name="exchange",
        )(*[pltpu.with_memory_space_constraint(x, pltpu.HBM) for x in operands])
        outs = [((slots, seq_len, rank), bf16), ((slots, rope_dim, seq_len), bf16), ((slots, heads, rank), bf16)]
        c_cache, kr_cache, o_lat = pl.pallas_call(
            functools.partial(finish_kernel, n, (rank + rope_dim) ** -0.5),
            out_shape=[jax.ShapeDtypeStruct(*out) for out in outs],
            in_specs=[vmem] * len(passed),
            out_specs=[hbm] * 3,
            scratch_shapes=[
                pltpu.VMEM((slots, heads, 1), f32),
                pltpu.VMEM((slots, heads, 1), f32),
                pltpu.VMEM((slots, heads, rank), bf16),
                pltpu.SemaphoreType.DMA((2 * slots + 1,)),
            ],
            compiler_params=pltpu.CompilerParams(vmem_limit_bytes=8 * 1024 * 1024),
            name="finish",
        )(*got)
        return c_cache, jnp.transpose(kr_cache, (0, 2, 1)), o_lat

    return jax.shard_map(local_step, mesh=mesh, in_specs=(seq_spec, seq_spec, P(None), P("x", None), P("x", None), P("dp"), req_spec, req_spec), out_specs=(req_spec, req_spec, req_spec), check_vma=False)
```

```python
import functools

import jax
import jax.numpy as jnp
from jax import lax
from jax.experimental import pallas as pl
from jax.experimental.pallas import tpu as pltpu
from jax.sharding import PartitionSpec as P

NORM_EPS = 1e-6
MASKED = -3.0e38
MESH = pl.DeviceIdType.MESH
DISTANCES = (3, 2, 1)
RAW = 2


def message_order(chips, slots):
    order = []
    for dist in DISTANCES:
        for core in (0, 1):
            for sign in (1, -1):
                order.append((sign * dist, core, 0, slots))
    order.insert(4, (0, 1, 0, slots))
    for core in (0, 1):
        order.append((chips // 2, core, 0, slots))
    return order


def normed_rows(rows, gain, first_pos, length):
    rows = rows.astype(jnp.float32)
    inv_rms = lax.rsqrt(jnp.mean(rows * rows, axis=-1, keepdims=True) + NORM_EPS)
    valid = first_pos + lax.broadcasted_iota(jnp.int32, (rows.shape[0], 1), 0) < length
    return jnp.where(valid, rows * inv_rms * gain, 0.0).astype(jnp.bfloat16)


def attend_chunk(r, chip, q_lat, rope_q, recv, kr_out, acc, top, total, own_lens, attn_scale):
    width = own_lens.shape[-1]
    start = pl.multiple_of(chip * width, width)
    rows = recv[r, pl.ds(start, width), :]
    keys = kr_out[r, :, pl.ds(start, width)]
    scores = lax.dot_general(q_lat[r], rows, (((1,), (1,)), ((), ())), preferred_element_type=jnp.float32)
    scores += jnp.dot(rope_q[r], keys, preferred_element_type=jnp.float32)
    pos = start + lax.broadcasted_iota(jnp.int32, (1, width), 1)
    valid = pos < own_lens[r]
    scores = jnp.where(valid, scores * attn_scale, MASKED)
    old_top = top[r]
    new_top = jnp.maximum(old_top, jnp.max(scores, axis=-1, keepdims=True))
    weights = jnp.where(valid, jnp.exp(scores - new_top), 0.0)
    decay = jnp.exp(old_top - new_top)
    top[r] = new_top
    new_total = total[r] * decay + jnp.sum(weights, axis=-1, keepdims=True)
    total[r] = new_total
    mixed = acc[r] * decay + jnp.dot(weights.astype(jnp.bfloat16), rows, preferred_element_type=jnp.float32)
    return mixed, new_total


def exchange_kernel(n, lens_hbm, lens_row_hbm, gain_hbm, cos_hbm, sin_hbm, c_hbm, k_hbm, ql_hbm, qr_hbm, recv, kr_out, acc, top, total, q_lat, rope_q, own_lens, lens, lens_row, gain_ref, cos_ref, sin_ref, send, k_raw, rot, turned, kr_send, kr_recv, q_rope, small_sem, load_sem, send_sem, recv_sem, kr_send_sem, kr_recv_sem):
    me = lax.axis_index("x")
    chips = n // 2
    my_chip, my_core = me // 2, lax.rem(me, 2)
    _, slots, seq_local, rank = send.shape
    half = cos_ref.shape[0]
    attn_scale = (rank + 2 * half) ** -0.5
    messages = message_order(chips, slots)

    def device(dist, core):
        return 2 * lax.rem(my_chip + dist + chips, chips) + lax.rem(my_core + core, 2)

    partners = []
    for dist, core, _, _ in messages:
        if (dist, core) not in partners:
            partners.append((dist, core))
    targets = [device(*partner) for partner in partners]

    barrier = pltpu.get_barrier_semaphore()
    for target in targets:
        pl.semaphore_signal(barrier, inc=1, device_id={"x": target}, device_id_type=MESH)

    def load_c(i):
        dest = me if i == n - 1 else targets[i]
        return pltpu.make_async_copy(c_hbm.at[dest], send.at[dest], load_sem.at[i])

    small = [(lens_hbm, lens), (gain_hbm, gain_ref), (lens_row_hbm, lens_row), (cos_hbm, cos_ref), (sin_hbm, sin_ref), (k_hbm, k_raw), (qr_hbm, q_rope), (ql_hbm, q_lat)]
    small = [pltpu.make_async_copy(src, dst, small_sem.at[i]) for i, (src, dst) in enumerate(small)]

    def norm_rows(dest, first, count):
        def one(slot, carry):
            normed = normed_rows(send[dest, slot], gain, me * seq_local, lens[dest * slots + slot])
            if dest is me:
                recv[slot, pl.ds(pl.multiple_of(me * seq_local, seq_local), seq_local), :] = normed
            else:
                send[dest, slot] = normed
            return carry

        lax.fori_loop(first, first + count, one, 0, unroll=2)

    def c_copy(m):
        dist, core, first, count = messages[m]
        target = device(dist, core)
        return pltpu.make_async_remote_copy(
            src_ref=(c_hbm if m < RAW else send).at[target, pl.ds(first, count)],
            dst_ref=recv.at[pl.ds(first, count), pl.ds(pl.multiple_of(me * seq_local, seq_local), seq_local)],
            send_sem=send_sem.at[m],
            recv_sem=recv_sem.at[m],
            device_id={"x": target},
            device_id_type=MESH,
        )

    def kr_copy(i):
        return pltpu.make_async_remote_copy(
            src_ref=kr_send.at[targets[i]],
            dst_ref=kr_recv.at[me],
            send_sem=kr_send_sem.at[i],
            recv_sem=kr_recv_sem.at[i],
            device_id={"x": targets[i]},
            device_id_type=MESH,
        )

    loaded = []

    def send_rows(m):
        dist, core, first, count = messages[m]
        if m >= RAW:
            i = partners.index((dist, core))
            if i not in loaded:
                load_c(i).wait()
                loaded.append(i)
            norm_rows(targets[i], first, count)
        c_copy(m).start()
        if m >= RAW and first == 0:
            kr_copy(partners.index((dist, core))).start()

    for copy in small[:2]:
        copy.start()
    loads = [i for i in range(n) if i == n - 1 or any(partners[i] == message[:2] for message in messages[RAW:])]
    for i in loads[:3]:
        load_c(i).start()
    for copy in small[2:]:
        copy.start()
    for i in loads[3:]:
        load_c(i).start()

    pl.semaphore_wait(barrier, n - 1)
    for m in range(RAW):
        send_rows(m)
    for copy in small:
        copy.wait()
    lens_vec = lens_row[...]
    for pos in range(seq_local):
        lo = k_raw[pos, :half, :].astype(jnp.float32)
        hi = k_raw[pos, half:, :].astype(jnp.float32)
        cos = cos_ref[:, pos : pos + 1]
        sin = sin_ref[:, pos : pos + 1]
        valid = me * seq_local + pos < lens_vec
        rot[2 * half * pos : 2 * half * pos + half, :] = jnp.where(valid, lo * cos - hi * sin, 0.0)
        rot[2 * half * pos + half : 2 * half * (pos + 1), :] = jnp.where(valid, hi * cos + lo * sin, 0.0)
    requests = n * slots
    for dim in range(half):
        lo = rot[pl.ds(dim, seq_local, stride=2 * half), :]
        hi = rot[pl.ds(half + dim, seq_local, stride=2 * half), :]
        turned[pl.ds(dim, requests, stride=half), :] = jnp.concatenate([lo, hi], axis=0).T
    for dest in range(n):
        kr_send[dest] = turned[dest * slots * half : (dest + 1) * slots * half, :].astype(jnp.bfloat16)
    kr_recv[me] = kr_send[me]

    for i in range(RAW):
        kr_copy(i).start()
    gain = gain_ref[...].astype(jnp.float32).reshape(1, rank)
    for m in range(RAW, len(messages)):
        send_rows(m)
    load_c(n - 1).wait()
    norm_rows(me, 0, slots)

    for slot in range(slots):
        rope_q[slot] = q_rope[slot].astype(jnp.float32).T.astype(jnp.bfloat16)
        own_lens[slot] = jnp.full(own_lens.shape[1:], lens[me * slots + slot], jnp.int32)
    acc[...] = jnp.zeros_like(acc)
    top[...] = jnp.full_like(top, MASKED)
    total[...] = jnp.zeros_like(total)

    low_lanes = lax.broadcasted_iota(jnp.int32, (half, 2 * seq_local), 1) < seq_local

    def gather_chip(dist):
        chip = lax.rem(my_chip + dist + chips, chips)
        for i, (far, _) in enumerate(partners):
            if (far + dist) % chips == 0:
                kr_copy(i).wait_recv()
        start = pl.multiple_of(chip * 2 * seq_local, 2 * seq_local)
        for slot in range(slots):
            even = kr_recv[2 * chip, slot * half : (slot + 1) * half, :].astype(jnp.float32)
            odd = kr_recv[2 * chip + 1, slot * half : (slot + 1) * half, :].astype(jnp.float32)
            kr_out[slot, :half, pl.ds(start, 2 * seq_local)] = jnp.where(low_lanes, even, pltpu.roll(odd, seq_local, 1)).astype(jnp.bfloat16)
            kr_out[slot, half:, pl.ds(start, 2 * seq_local)] = jnp.where(low_lanes, pltpu.roll(even, seq_local, 1), odd).astype(jnp.bfloat16)
        for m, (far, _, _, _) in enumerate(messages):
            if (far + dist) % chips == 0:
                c_copy(m).wait_recv()
                if m < RAW:
                    first_pos = pl.multiple_of((2 * chip + lax.rem(my_core + messages[m][1], 2)) * seq_local, seq_local)

                    def one(slot, carry, first_pos=first_pos):
                        recv[slot, pl.ds(first_pos, seq_local), :] = normed_rows(recv[slot, pl.ds(first_pos, seq_local), :], gain, first_pos, lens[me * slots + slot])
                        return carry

                    lax.fori_loop(messages[m][2], sum(messages[m][2:]), one, 0, unroll=2)
        return chip

    for dist in [0] + [sign * far for far in DISTANCES for sign in (1, -1)]:
        chip = gather_chip(dist)

        def one_request(r, carry, chip=chip):
            acc[r], _ = attend_chunk(r, chip, q_lat, rope_q, recv, kr_out, acc, top, total, own_lens, attn_scale)
            return carry

        lax.fori_loop(0, slots, one_request, 0, unroll=2)

    for i in range(n - 1):
        kr_copy(i).wait_send()
    gather_chip(chips // 2)
    for m in range(len(messages)):
        c_copy(m).wait_send()


def finish_kernel(n, attn_scale, recv, kr_in, acc, top_in, total_in, q_lat, rope_q, own_lens, c_out, kr_out, o_out, top, total, o_ref, sem):
    chips = n // 2
    slots = acc.shape[0]
    copies = [pltpu.make_async_copy(recv.at[r], c_out.at[r], sem.at[r]) for r in range(slots)]
    copies.append(pltpu.make_async_copy(kr_in, kr_out, sem.at[slots]))
    for copy in copies:
        copy.start()
    top[...] = top_in[...]
    total[...] = total_in[...]
    chip = lax.rem(lax.axis_index("x") // 2 + chips // 2, chips)
    for r in range(slots):
        mixed, weight_sum = attend_chunk(r, chip, q_lat, rope_q, recv, kr_in, acc, top, total, own_lens, attn_scale)
        o_ref[r] = (mixed / weight_sum).astype(jnp.bfloat16)
        copies.append(pltpu.make_async_copy(o_ref.at[r], o_out.at[r], sem.at[slots + 1 + r]))
        copies[-1].start()
    for copy in copies:
        copy.wait()


def solution(mesh):
    n = mesh.shape["x"]
    seq_spec = P("dp", "x", None)
    req_spec = P(("dp", "x"), None, None)

    def local_step(c_raw, k_raw, norm_gain, rope_cos, rope_sin, seq_lens, q_lat, q_rope):
        requests, seq_local, rank = c_raw.shape
        slots, heads, _ = q_lat.shape
        rope_dim = k_raw.shape[-1]
        half = rope_dim // 2
        seq_len = n * seq_local
        bf16, f32, i32 = jnp.bfloat16, jnp.float32, jnp.int32
        hbm = pl.BlockSpec(memory_space=pltpu.HBM)
        vmem = pl.BlockSpec(memory_space=pltpu.VMEM)
        messages = len(message_order(n // 2, slots))
        passed = [
            ((slots, seq_len, rank), bf16),
            ((slots, rope_dim, seq_len), bf16),
            ((slots, heads, rank), f32),
            ((slots, heads, 1), f32),
            ((slots, heads, 1), f32),
            ((slots, heads, rank), bf16),
            ((slots, heads, rope_dim), bf16),
            ((slots, 1, 2 * seq_local), i32),
        ]
        operands = (
            seq_lens,
            seq_lens.reshape(1, requests),
            norm_gain,
            rope_cos.T,
            rope_sin.T,
            c_raw.reshape(n, slots, seq_local, rank),
            jnp.transpose(k_raw, (1, 2, 0)),
            q_lat,
            jnp.transpose(q_rope, (0, 2, 1)),
        )
        got = pl.pallas_call(
            functools.partial(exchange_kernel, n),
            out_shape=[pltpu.VMEM(*out) for out in passed],
            in_specs=[hbm] * len(operands),
            out_specs=[vmem] * len(passed),
            scratch_shapes=[
                pltpu.SMEM((requests,), i32),
                pltpu.VMEM((1, requests), i32),
                pltpu.VMEM((rank,), bf16),
                pltpu.VMEM((half, seq_local), f32),
                pltpu.VMEM((half, seq_local), f32),
                pltpu.VMEM((n, slots, seq_local, rank), bf16),
                pltpu.VMEM((seq_local, rope_dim, requests), bf16),
                pltpu.VMEM((seq_local * rope_dim, requests), f32),
                pltpu.VMEM((requests * half, 2 * seq_local), f32),
                pltpu.VMEM((n, slots * half, 2 * seq_local), bf16),
                pltpu.VMEM((n, slots * half, 2 * seq_local), bf16),
                pltpu.VMEM((slots, rope_dim, heads), bf16),
                pltpu.SemaphoreType.DMA((8,)),
                pltpu.SemaphoreType.DMA((n,)),
                pltpu.SemaphoreType.DMA((messages,)),
                pltpu.SemaphoreType.DMA((messages,)),
                pltpu.SemaphoreType.DMA((n - 1,)),
                pltpu.SemaphoreType.DMA((n - 1,)),
            ],
            compiler_params=pltpu.CompilerParams(collective_id=0, has_side_effects=True, vmem_limit_bytes=40 * 1024 * 1024),
            name="exchange",
        )(*[pltpu.with_memory_space_constraint(x, pltpu.HBM) for x in operands])
        outs = [((slots, seq_len, rank), bf16), ((slots, rope_dim, seq_len), bf16), ((slots, heads, rank), bf16)]
        c_cache, kr_cache, o_lat = pl.pallas_call(
            functools.partial(finish_kernel, n, (rank + rope_dim) ** -0.5),
            out_shape=[jax.ShapeDtypeStruct(*out) for out in outs],
            in_specs=[vmem] * len(passed),
            out_specs=[hbm] * 3,
            scratch_shapes=[
                pltpu.VMEM((slots, heads, 1), f32),
                pltpu.VMEM((slots, heads, 1), f32),
                pltpu.VMEM((slots, heads, rank), bf16),
                pltpu.SemaphoreType.DMA((2 * slots + 1,)),
            ],
            compiler_params=pltpu.CompilerParams(vmem_limit_bytes=8 * 1024 * 1024),
            name="finish",
        )(*got)
        return c_cache, jnp.transpose(kr_cache, (0, 2, 1)), o_lat

    return jax.shard_map(local_step, mesh=mesh, in_specs=(seq_spec, seq_spec, P(None), P("x", None), P("x", None), P("dp"), req_spec, req_spec), out_specs=(req_spec, req_spec, req_spec), check_vma=False)
```

```python
import functools

import jax
import jax.numpy as jnp
from jax import lax
from jax.experimental import pallas as pl
from jax.experimental.pallas import tpu as pltpu
from jax.sharding import PartitionSpec as P

NORM_EPS = 1e-6
MASKED = -3.0e38
MESH = pl.DeviceIdType.MESH
DISTANCES = (3, 2, 1)
RAW = 2


def message_order(chips, slots):
    order = []
    for dist in DISTANCES:
        for core in (0, 1):
            for sign in (1, -1):
                order.append((sign * dist, core, 0, slots))
    order.insert(4, (0, 1, 0, slots))
    for core in (0, 1):
        order.append((chips // 2, core, 0, slots))
    return order


def normed_rows(rows, gain, first_pos, length):
    rows = rows.astype(jnp.float32)
    inv_rms = lax.rsqrt(jnp.mean(rows * rows, axis=-1, keepdims=True) + NORM_EPS)
    valid = first_pos + lax.broadcasted_iota(jnp.int32, (rows.shape[0], 1), 0) < length
    return jnp.where(valid, rows * inv_rms * gain, 0.0).astype(jnp.bfloat16)


def attend_chunk(r, chip, q_lat, rope_q, recv, kr_out, acc, top, total, own_lens, attn_scale):
    width = own_lens.shape[-1]
    start = pl.multiple_of(chip * width, width)
    rows = recv[r, pl.ds(start, width), :]
    keys = kr_out[r, :, pl.ds(start, width)]
    scores = lax.dot_general(q_lat[r], rows, (((1,), (1,)), ((), ())), preferred_element_type=jnp.float32)
    scores += jnp.dot(rope_q[r], keys, preferred_element_type=jnp.float32)
    pos = start + lax.broadcasted_iota(jnp.int32, (1, width), 1)
    valid = pos < own_lens[r]
    scores = jnp.where(valid, scores * attn_scale, MASKED)
    old_top = top[r]
    new_top = jnp.maximum(old_top, jnp.max(scores, axis=-1, keepdims=True))
    weights = jnp.where(valid, jnp.exp(scores - new_top), 0.0)
    decay = jnp.exp(old_top - new_top)
    top[r] = new_top
    new_total = total[r] * decay + jnp.sum(weights, axis=-1, keepdims=True)
    total[r] = new_total
    mixed = acc[r] * decay + jnp.dot(weights.astype(jnp.bfloat16), rows, preferred_element_type=jnp.float32)
    return mixed, new_total


def exchange_kernel(n, lens_hbm, lens_row_hbm, gain_hbm, cos_hbm, sin_hbm, c_hbm, k_hbm, ql_hbm, qr_hbm, recv, kr_out, acc, top, total, q_lat, rope_q, own_lens, lens, lens_row, gain_ref, cos_ref, sin_ref, send, k_raw, rot, turned, kr_send, kr_recv, q_rope, small_sem, load_sem, send_sem, recv_sem, kr_send_sem, kr_recv_sem):
    me = lax.axis_index("x")
    chips = n // 2
    my_chip, my_core = me // 2, lax.rem(me, 2)
    _, slots, seq_local, rank = send.shape
    half = cos_ref.shape[0]
    attn_scale = (rank + 2 * half) ** -0.5
    messages = message_order(chips, slots)

    def device(dist, core):
        return 2 * lax.rem(my_chip + dist + chips, chips) + lax.rem(my_core + core, 2)

    partners = []
    for dist, core, _, _ in messages:
        if (dist, core) not in partners:
            partners.append((dist, core))
    targets = [device(*partner) for partner in partners]

    barrier = pltpu.get_barrier_semaphore()
    for target in targets:
        pl.semaphore_signal(barrier, inc=1, device_id={"x": target}, device_id_type=MESH)

    def load_c(i):
        dest = me if i == n - 1 else targets[i]
        return pltpu.make_async_copy(c_hbm.at[dest], send.at[dest], load_sem.at[0])

    small = [(lens_hbm, lens), (gain_hbm, gain_ref), (lens_row_hbm, lens_row), (cos_hbm, cos_ref), (sin_hbm, sin_ref), (k_hbm, k_raw), (qr_hbm, q_rope), (ql_hbm, q_lat)]
    small = [pltpu.make_async_copy(src, dst, small_sem.at[i]) for i, (src, dst) in enumerate(small)]

    def norm_rows(dest, first, count):
        def one(slot, carry):
            normed = normed_rows(send[dest, slot], gain, me * seq_local, lens[dest * slots + slot])
            if dest is me:
                recv[slot, pl.ds(pl.multiple_of(me * seq_local, seq_local), seq_local), :] = normed
            else:
                send[dest, slot] = normed
            return carry

        lax.fori_loop(first, first + count, one, 0, unroll=2)

    def c_copy(m):
        dist, core, first, count = messages[m]
        target = device(dist, core)
        return pltpu.make_async_remote_copy(
            src_ref=(c_hbm if m < RAW else send).at[target, pl.ds(first, count)],
            dst_ref=recv.at[pl.ds(first, count), pl.ds(pl.multiple_of(me * seq_local, seq_local), seq_local)],
            send_sem=send_sem.at[0],
            recv_sem=recv_sem.at[dist % chips],
            device_id={"x": target},
            device_id_type=MESH,
        )

    def kr_copy(i):
        return pltpu.make_async_remote_copy(
            src_ref=kr_send.at[targets[i]],
            dst_ref=kr_recv.at[me],
            send_sem=kr_send_sem.at[0],
            recv_sem=kr_recv_sem.at[partners[i][0] % chips],
            device_id={"x": targets[i]},
            device_id_type=MESH,
        )

    def wait_for(region, sem):
        pltpu.make_async_copy(region, region, sem).wait()

    def send_rows(m):
        dist, core, first, count = messages[m]
        if m >= RAW:
            i = partners.index((dist, core))
            norm_rows(targets[i], first, count)
            kr_copy(i).start()
        c_copy(m).start()

    for copy in small[:2]:
        copy.start()
    loads = [i for i in range(n) if i == n - 1 or any(partners[i] == message[:2] for message in messages[RAW:])]
    for i in loads[:3]:
        load_c(i).start()
    for copy in small[2:]:
        copy.start()
    for i in loads[3:]:
        load_c(i).start()

    pl.semaphore_wait(barrier, n - 1)
    for m in range(RAW):
        send_rows(m)
    for copy in small:
        copy.wait()
    lens_vec = lens_row[...]
    for pos in range(seq_local):
        lo = k_raw[pos, :half, :].astype(jnp.float32)
        hi = k_raw[pos, half:, :].astype(jnp.float32)
        cos = cos_ref[:, pos : pos + 1]
        sin = sin_ref[:, pos : pos + 1]
        valid = me * seq_local + pos < lens_vec
        rot[2 * half * pos : 2 * half * pos + half, :] = jnp.where(valid, lo * cos - hi * sin, 0.0)
        rot[2 * half * pos + half : 2 * half * (pos + 1), :] = jnp.where(valid, hi * cos + lo * sin, 0.0)
    requests = n * slots
    for dim in range(half):
        lo = rot[pl.ds(dim, seq_local, stride=2 * half), :]
        hi = rot[pl.ds(half + dim, seq_local, stride=2 * half), :]
        turned[pl.ds(dim, requests, stride=half), :] = jnp.concatenate([lo, hi], axis=0).T
    for dest in range(n):
        kr_send[dest] = turned[dest * slots * half : (dest + 1) * slots * half, :].astype(jnp.bfloat16)
    kr_recv[me] = kr_send[me]

    for i in range(RAW):
        kr_copy(i).start()
    gain = gain_ref[...].astype(jnp.float32).reshape(1, rank)
    wait_for(send.at[pl.ds(0, len(loads))], load_sem.at[0])
    for m in range(RAW, len(messages)):
        send_rows(m)
    norm_rows(me, 0, slots)

    for slot in range(slots):
        rope_q[slot] = q_rope[slot].astype(jnp.float32).T.astype(jnp.bfloat16)
        own_lens[slot] = jnp.full(own_lens.shape[1:], lens[me * slots + slot], jnp.int32)
    acc[...] = jnp.zeros_like(acc)
    top[...] = jnp.full_like(top, MASKED)
    total[...] = jnp.zeros_like(total)

    low_lanes = lax.broadcasted_iota(jnp.int32, (half, 2 * seq_local), 1) < seq_local

    def gather_chip(dist):
        chip = lax.rem(my_chip + dist + chips, chips)
        partner = device(0, 1)
        wait_for(kr_recv.at[pl.ds(2 * chip, 2)] if dist else kr_recv.at[partner], kr_recv_sem.at[-dist % chips])
        start = pl.multiple_of(chip * 2 * seq_local, 2 * seq_local)
        for slot in range(slots):
            even = kr_recv[2 * chip, slot * half : (slot + 1) * half, :].astype(jnp.float32)
            odd = kr_recv[2 * chip + 1, slot * half : (slot + 1) * half, :].astype(jnp.float32)
            kr_out[slot, :half, pl.ds(start, 2 * seq_local)] = jnp.where(low_lanes, even, pltpu.roll(odd, seq_local, 1)).astype(jnp.bfloat16)
            kr_out[slot, half:, pl.ds(start, 2 * seq_local)] = jnp.where(low_lanes, pltpu.roll(even, seq_local, 1), odd).astype(jnp.bfloat16)
        wait_for(recv.at[:, pl.ds(start, 2 * seq_local)] if dist else recv.at[:, pl.ds(pl.multiple_of(partner * seq_local, seq_local), seq_local)], recv_sem.at[-dist % chips])
        for m, (far, _, _, _) in enumerate(messages):
            if (far + dist) % chips == 0:
                if m < RAW:
                    first_pos = pl.multiple_of((2 * chip + lax.rem(my_core + messages[m][1], 2)) * seq_local, seq_local)

                    def one(slot, carry, first_pos=first_pos):
                        recv[slot, pl.ds(first_pos, seq_local), :] = normed_rows(recv[slot, pl.ds(first_pos, seq_local), :], gain, first_pos, lens[me * slots + slot])
                        return carry

                    lax.fori_loop(messages[m][2], sum(messages[m][2:]), one, 0, unroll=2)
        return chip

    for dist in [0] + [sign * far for far in DISTANCES for sign in (1, -1)]:
        chip = gather_chip(dist)

        def one_request(r, carry, chip=chip):
            acc[r], _ = attend_chunk(r, chip, q_lat, rope_q, recv, kr_out, acc, top, total, own_lens, attn_scale)
            return carry

        lax.fori_loop(0, slots, one_request, 0, unroll=2)

    gather_chip(chips // 2)
    wait_for(kr_send.at[pl.ds(0, n - 1)], kr_send_sem.at[0])
    wait_for(send.at[pl.ds(0, n - 1)], send_sem.at[0])


def finish_kernel(n, attn_scale, recv, kr_in, acc, top_in, total_in, q_lat, rope_q, own_lens, c_out, kr_out, o_out, top, total, o_ref, sem):
    chips = n // 2
    slots = acc.shape[0]
    copies = [pltpu.make_async_copy(recv.at[r], c_out.at[r], sem.at[r]) for r in range(slots)]
    copies.append(pltpu.make_async_copy(kr_in, kr_out, sem.at[slots]))
    for copy in copies:
        copy.start()
    top[...] = top_in[...]
    total[...] = total_in[...]
    chip = lax.rem(lax.axis_index("x") // 2 + chips // 2, chips)
    for r in range(slots):
        mixed, weight_sum = attend_chunk(r, chip, q_lat, rope_q, recv, kr_in, acc, top, total, own_lens, attn_scale)
        o_ref[r] = (mixed / weight_sum).astype(jnp.bfloat16)
        copies.append(pltpu.make_async_copy(o_ref.at[r], o_out.at[r], sem.at[slots + 1 + r]))
        copies[-1].start()
    for copy in copies:
        copy.wait()


def solution(mesh):
    n = mesh.shape["x"]
    seq_spec = P("dp", "x", None)
    req_spec = P(("dp", "x"), None, None)

    def local_step(c_raw, k_raw, norm_gain, rope_cos, rope_sin, seq_lens, q_lat, q_rope):
        requests, seq_local, rank = c_raw.shape
        slots, heads, _ = q_lat.shape
        rope_dim = k_raw.shape[-1]
        half = rope_dim // 2
        seq_len = n * seq_local
        bf16, f32, i32 = jnp.bfloat16, jnp.float32, jnp.int32
        hbm = pl.BlockSpec(memory_space=pltpu.HBM)
        vmem = pl.BlockSpec(memory_space=pltpu.VMEM)
        passed = [
            ((slots, seq_len, rank), bf16),
            ((slots, rope_dim, seq_len), bf16),
            ((slots, heads, rank), f32),
            ((slots, heads, 1), f32),
            ((slots, heads, 1), f32),
            ((slots, heads, rank), bf16),
            ((slots, heads, rope_dim), bf16),
            ((slots, 1, 2 * seq_local), i32),
        ]
        operands = (
            seq_lens,
            seq_lens.reshape(1, requests),
            norm_gain,
            rope_cos.T,
            rope_sin.T,
            c_raw.reshape(n, slots, seq_local, rank),
            jnp.transpose(k_raw, (1, 2, 0)),
            q_lat,
            jnp.transpose(q_rope, (0, 2, 1)),
        )
        got = pl.pallas_call(
            functools.partial(exchange_kernel, n),
            out_shape=[pltpu.VMEM(*out) for out in passed],
            in_specs=[hbm] * len(operands),
            out_specs=[vmem] * len(passed),
            scratch_shapes=[
                pltpu.SMEM((requests,), i32),
                pltpu.VMEM((1, requests), i32),
                pltpu.VMEM((rank,), bf16),
                pltpu.VMEM((half, seq_local), f32),
                pltpu.VMEM((half, seq_local), f32),
                pltpu.VMEM((n, slots, seq_local, rank), bf16),
                pltpu.VMEM((seq_local, rope_dim, requests), bf16),
                pltpu.VMEM((seq_local * rope_dim, requests), f32),
                pltpu.VMEM((requests * half, 2 * seq_local), f32),
                pltpu.VMEM((n, slots * half, 2 * seq_local), bf16),
                pltpu.VMEM((n, slots * half, 2 * seq_local), bf16),
                pltpu.VMEM((slots, rope_dim, heads), bf16),
                pltpu.SemaphoreType.DMA((8,)),
                pltpu.SemaphoreType.DMA((1,)),
                pltpu.SemaphoreType.DMA((1,)),
                pltpu.SemaphoreType.DMA((n // 2,)),
                pltpu.SemaphoreType.DMA((1,)),
                pltpu.SemaphoreType.DMA((n // 2,)),
            ],
            compiler_params=pltpu.CompilerParams(collective_id=0, has_side_effects=True, vmem_limit_bytes=40 * 1024 * 1024),
            name="exchange",
        )(*[pltpu.with_memory_space_constraint(x, pltpu.HBM) for x in operands])
        outs = [((slots, seq_len, rank), bf16), ((slots, rope_dim, seq_len), bf16), ((slots, heads, rank), bf16)]
        c_cache, kr_cache, o_lat = pl.pallas_call(
            functools.partial(finish_kernel, n, (rank + rope_dim) ** -0.5),
            out_shape=[jax.ShapeDtypeStruct(*out) for out in outs],
            in_specs=[vmem] * len(passed),
            out_specs=[hbm] * 3,
            scratch_shapes=[
                pltpu.VMEM((slots, heads, 1), f32),
                pltpu.VMEM((slots, heads, 1), f32),
                pltpu.VMEM((slots, heads, rank), bf16),
                pltpu.SemaphoreType.DMA((2 * slots + 1,)),
            ],
            compiler_params=pltpu.CompilerParams(vmem_limit_bytes=8 * 1024 * 1024),
            name="finish",
        )(*got)
        return c_cache, jnp.transpose(kr_cache, (0, 2, 1)), o_lat

    return jax.shard_map(local_step, mesh=mesh, in_specs=(seq_spec, seq_spec, P(None), P("x", None), P("x", None), P("dp"), req_spec, req_spec), out_specs=(req_spec, req_spec, req_spec), check_vma=False)
```

```python
import functools

import jax
import jax.numpy as jnp
from jax import lax
from jax.experimental import pallas as pl
from jax.experimental.pallas import tpu as pltpu
from jax.sharding import PartitionSpec as P

NORM_EPS = 1e-6
MASKED = -3.0e38
MESH = pl.DeviceIdType.MESH
DISTANCES = (3, 2, 1)
RAW = 2


def message_order(chips, slots):
    order = []
    for dist in DISTANCES:
        for core in (0, 1):
            for sign in (1, -1):
                order.append((sign * dist, core, 0, slots))
    order.insert(4, (0, 1, 0, slots))
    for core in (0, 1):
        order.append((chips // 2, core, 0, slots))
    return order


def normed_rows(rows, gain, first_pos, length):
    rows = rows.astype(jnp.float32)
    inv_rms = lax.rsqrt(jnp.mean(rows * rows, axis=-1, keepdims=True) + NORM_EPS)
    valid = first_pos + lax.broadcasted_iota(jnp.int32, (rows.shape[0], 1), 0) < length
    return jnp.where(valid, rows * inv_rms * gain, 0.0).astype(jnp.bfloat16)


def attend_chunk(r, chip, q_lat, rope_q, recv, kr_out, acc, top, total, own_lens, attn_scale):
    width = own_lens.shape[-1]
    start = pl.multiple_of(chip * width, width)
    rows = recv[r, pl.ds(start, width), :]
    keys = kr_out[r, :, pl.ds(start, width)]
    scores = lax.dot_general(q_lat[r], rows, (((1,), (1,)), ((), ())), preferred_element_type=jnp.float32)
    scores += jnp.dot(rope_q[r], keys, preferred_element_type=jnp.float32)
    pos = start + lax.broadcasted_iota(jnp.int32, (1, width), 1)
    valid = pos < own_lens[r]
    scores = jnp.where(valid, scores * attn_scale, MASKED)
    old_top = top[r]
    new_top = jnp.maximum(old_top, jnp.max(scores, axis=-1, keepdims=True))
    weights = jnp.where(valid, jnp.exp(scores - new_top), 0.0)
    decay = jnp.exp(old_top - new_top)
    top[r] = new_top
    new_total = total[r] * decay + jnp.sum(weights, axis=-1, keepdims=True)
    total[r] = new_total
    mixed = acc[r] * decay + jnp.dot(weights.astype(jnp.bfloat16), rows, preferred_element_type=jnp.float32)
    return mixed, new_total


def exchange_kernel(n, lens_hbm, lens_row_hbm, gain_hbm, cos_hbm, sin_hbm, c_hbm, k_hbm, ql_hbm, qr_hbm, recv, kr_out, acc, top, total, q_lat, rope_q, own_lens, lens, lens_row, gain_ref, cos_ref, sin_ref, send, k_raw, rot, turned, kr_send, kr_recv, q_rope, small_sem, load_sem, send_sem, recv_sem, kr_send_sem, kr_recv_sem):
    me = lax.axis_index("x")
    chips = n // 2
    my_chip, my_core = me // 2, lax.rem(me, 2)
    _, slots, seq_local, rank = send.shape
    half = cos_ref.shape[0]
    attn_scale = (rank + 2 * half) ** -0.5
    messages = message_order(chips, slots)

    def device(dist, core):
        return 2 * lax.rem(my_chip + dist + chips, chips) + lax.rem(my_core + core, 2)

    partners = []
    for dist, core, _, _ in messages:
        if (dist, core) not in partners:
            partners.append((dist, core))
    targets = [device(*partner) for partner in partners]

    barrier = pltpu.get_barrier_semaphore()
    for target in targets:
        pl.semaphore_signal(barrier, inc=1, device_id={"x": target}, device_id_type=MESH)

    def load_c(i):
        dest = me if i == n - 1 else targets[i]
        return pltpu.make_async_copy(c_hbm.at[dest], send.at[dest], load_sem.at[0])

    small = [(lens_hbm, lens), (gain_hbm, gain_ref), (lens_row_hbm, lens_row), (cos_hbm, cos_ref), (sin_hbm, sin_ref), (k_hbm, k_raw), (qr_hbm, q_rope), (ql_hbm, q_lat)]
    small = [pltpu.make_async_copy(src, dst, small_sem.at[i]) for i, (src, dst) in enumerate(small)]

    def norm_rows(dest, first, count):
        def one(slot, carry):
            normed = normed_rows(send[dest, slot], gain, me * seq_local, lens[dest * slots + slot])
            if dest is me:
                recv[slot, pl.ds(pl.multiple_of(me * seq_local, seq_local), seq_local), :] = normed
            else:
                send[dest, slot] = normed
            return carry

        lax.fori_loop(first, first + count, one, 0, unroll=2)

    def c_copy(m):
        dist, core, first, count = messages[m]
        target = device(dist, core)
        return pltpu.make_async_remote_copy(
            src_ref=(c_hbm if m < RAW else send).at[target, pl.ds(first, count)],
            dst_ref=recv.at[pl.ds(first, count), pl.ds(pl.multiple_of(me * seq_local, seq_local), seq_local)],
            send_sem=send_sem.at[0],
            recv_sem=recv_sem.at[dist % chips],
            device_id={"x": target},
            device_id_type=MESH,
        )

    def kr_copy(i):
        return pltpu.make_async_remote_copy(
            src_ref=kr_send.at[targets[i]],
            dst_ref=kr_recv.at[me],
            send_sem=kr_send_sem.at[0],
            recv_sem=kr_recv_sem.at[partners[i][0] % chips],
            device_id={"x": targets[i]},
            device_id_type=MESH,
        )

    def wait_for(region, sem):
        pltpu.make_async_copy(region, region, sem).wait()

    def send_rows(m):
        dist, core, first, count = messages[m]
        if m >= RAW:
            i = partners.index((dist, core))
            norm_rows(targets[i], first, count)
            kr_copy(i).start()
        c_copy(m).start()

    for copy in small[:2]:
        copy.start()
    loads = [i for i in range(n) if i == n - 1 or any(partners[i] == message[:2] for message in messages[RAW:])]
    for i in loads[:3]:
        load_c(i).start()
    for copy in small[2:]:
        copy.start()
    for i in loads[3:]:
        load_c(i).start()

    pl.semaphore_wait(barrier, n - 1)
    for m in range(RAW):
        send_rows(m)
    for copy in small:
        copy.wait()
    lens_vec = lens_row[...]
    for pos in range(seq_local):
        lo = k_raw[pos, :half, :].astype(jnp.float32)
        hi = k_raw[pos, half:, :].astype(jnp.float32)
        cos = cos_ref[:, pos : pos + 1]
        sin = sin_ref[:, pos : pos + 1]
        valid = me * seq_local + pos < lens_vec
        rot[2 * half * pos : 2 * half * pos + half, :] = jnp.where(valid, lo * cos - hi * sin, 0.0)
        rot[2 * half * pos + half : 2 * half * (pos + 1), :] = jnp.where(valid, hi * cos + lo * sin, 0.0)
    requests = n * slots
    for dim in range(half):
        lo = rot[pl.ds(dim, seq_local, stride=2 * half), :]
        hi = rot[pl.ds(half + dim, seq_local, stride=2 * half), :]
        turned[pl.ds(dim, requests, stride=half), :] = jnp.concatenate([lo, hi], axis=0).T
    for dest in range(n):
        kr_send[dest] = turned[dest * slots * half : (dest + 1) * slots * half, :].astype(jnp.bfloat16)
    kr_recv[me] = kr_send[me]

    for i in range(RAW):
        kr_copy(i).start()
    gain = gain_ref[...].astype(jnp.float32).reshape(1, rank)
    wait_for(send.at[pl.ds(0, len(loads))], load_sem.at[0])
    for m in range(RAW, len(messages)):
        send_rows(m)
    norm_rows(me, 0, slots)

    for slot in range(slots):
        rope_q[slot] = q_rope[slot].astype(jnp.float32).T.astype(jnp.bfloat16)
        own_lens[slot] = jnp.full(own_lens.shape[1:], lens[me * slots + slot], jnp.int32)
    acc[...] = jnp.zeros_like(acc)
    top[...] = jnp.full_like(top, MASKED)
    total[...] = jnp.zeros_like(total)

    low_lanes = lax.broadcasted_iota(jnp.int32, (half, 2 * seq_local), 1) < seq_local

    def gather_chip(dist):
        chip = lax.rem(my_chip + dist + chips, chips)
        partner = device(0, 1)
        wait_for(kr_recv.at[pl.ds(2 * chip, 2)] if dist else kr_recv.at[partner], kr_recv_sem.at[-dist % chips])
        start = pl.multiple_of(chip * 2 * seq_local, 2 * seq_local)
        for slot in range(slots):
            even = kr_recv[2 * chip, slot * half : (slot + 1) * half, :].astype(jnp.float32)
            odd = kr_recv[2 * chip + 1, slot * half : (slot + 1) * half, :].astype(jnp.float32)
            kr_out[slot, :half, pl.ds(start, 2 * seq_local)] = jnp.where(low_lanes, even, pltpu.roll(odd, seq_local, 1)).astype(jnp.bfloat16)
            kr_out[slot, half:, pl.ds(start, 2 * seq_local)] = jnp.where(low_lanes, pltpu.roll(even, seq_local, 1), odd).astype(jnp.bfloat16)
        wait_for(recv.at[:, pl.ds(start, 2 * seq_local)] if dist else recv.at[:, pl.ds(pl.multiple_of(partner * seq_local, seq_local), seq_local)], recv_sem.at[-dist % chips])
        for m, (far, _, _, _) in enumerate(messages):
            if (far + dist) % chips == 0:
                if m < RAW:
                    first_pos = pl.multiple_of((2 * chip + lax.rem(my_core + messages[m][1], 2)) * seq_local, seq_local)

                    def one(slot, carry, first_pos=first_pos):
                        recv[slot, pl.ds(first_pos, seq_local), :] = normed_rows(recv[slot, pl.ds(first_pos, seq_local), :], gain, first_pos, lens[me * slots + slot])
                        return carry

                    lax.fori_loop(messages[m][2], sum(messages[m][2:]), one, 0, unroll=2)
        return chip

    for dist in [0] + [sign * far for far in DISTANCES for sign in (1, -1)]:
        chip = gather_chip(dist)

        def one_request(r, carry, chip=chip):
            acc[r], _ = attend_chunk(r, chip, q_lat, rope_q, recv, kr_out, acc, top, total, own_lens, attn_scale)
            return carry

        lax.fori_loop(0, slots, one_request, 0, unroll=2)

    gather_chip(chips // 2)
    wait_for(kr_send.at[pl.ds(0, n - 1)], kr_send_sem.at[0])
    wait_for(send.at[pl.ds(0, n - 1)], send_sem.at[0])


def finish_kernel(n, attn_scale, recv, kr_in, acc, top_in, total_in, q_lat, rope_q, own_lens, c_out, kr_out, o_out, top, total, o_ref, sem):
    chips = n // 2
    slots = acc.shape[0]
    for r in range(slots):
        pltpu.make_async_copy(recv.at[r], c_out.at[r], sem.at[0]).start()
    pltpu.make_async_copy(kr_in, kr_out, sem.at[1]).start()
    top[...] = top_in[...]
    total[...] = total_in[...]
    chip = lax.rem(lax.axis_index("x") // 2 + chips // 2, chips)
    for r in range(slots):
        mixed, weight_sum = attend_chunk(r, chip, q_lat, rope_q, recv, kr_in, acc, top, total, own_lens, attn_scale)
        o_ref[r] = (mixed / weight_sum).astype(jnp.bfloat16)
        pltpu.make_async_copy(o_ref.at[r], o_out.at[r], sem.at[2]).start()
    for i, (src, dst) in enumerate([(recv, c_out), (kr_in, kr_out), (o_ref, o_out)]):
        pltpu.make_async_copy(src, dst, sem.at[i]).wait()


def solution(mesh):
    n = mesh.shape["x"]
    seq_spec = P("dp", "x", None)
    req_spec = P(("dp", "x"), None, None)

    def local_step(c_raw, k_raw, norm_gain, rope_cos, rope_sin, seq_lens, q_lat, q_rope):
        requests, seq_local, rank = c_raw.shape
        slots, heads, _ = q_lat.shape
        rope_dim = k_raw.shape[-1]
        half = rope_dim // 2
        seq_len = n * seq_local
        bf16, f32, i32 = jnp.bfloat16, jnp.float32, jnp.int32
        hbm = pl.BlockSpec(memory_space=pltpu.HBM)
        vmem = pl.BlockSpec(memory_space=pltpu.VMEM)
        passed = [
            ((slots, seq_len, rank), bf16),
            ((slots, rope_dim, seq_len), bf16),
            ((slots, heads, rank), f32),
            ((slots, heads, 1), f32),
            ((slots, heads, 1), f32),
            ((slots, heads, rank), bf16),
            ((slots, heads, rope_dim), bf16),
            ((slots, 1, 2 * seq_local), i32),
        ]
        operands = (
            seq_lens,
            seq_lens.reshape(1, requests),
            norm_gain,
            rope_cos.T,
            rope_sin.T,
            c_raw.reshape(n, slots, seq_local, rank),
            jnp.transpose(k_raw, (1, 2, 0)),
            q_lat,
            jnp.transpose(q_rope, (0, 2, 1)),
        )
        got = pl.pallas_call(
            functools.partial(exchange_kernel, n),
            out_shape=[pltpu.VMEM(*out) for out in passed],
            in_specs=[hbm] * len(operands),
            out_specs=[vmem] * len(passed),
            scratch_shapes=[
                pltpu.SMEM((requests,), i32),
                pltpu.VMEM((1, requests), i32),
                pltpu.VMEM((rank,), bf16),
                pltpu.VMEM((half, seq_local), f32),
                pltpu.VMEM((half, seq_local), f32),
                pltpu.VMEM((n, slots, seq_local, rank), bf16),
                pltpu.VMEM((seq_local, rope_dim, requests), bf16),
                pltpu.VMEM((seq_local * rope_dim, requests), f32),
                pltpu.VMEM((requests * half, 2 * seq_local), f32),
                pltpu.VMEM((n, slots * half, 2 * seq_local), bf16),
                pltpu.VMEM((n, slots * half, 2 * seq_local), bf16),
                pltpu.VMEM((slots, rope_dim, heads), bf16),
                pltpu.SemaphoreType.DMA((8,)),
                pltpu.SemaphoreType.DMA((1,)),
                pltpu.SemaphoreType.DMA((1,)),
                pltpu.SemaphoreType.DMA((n // 2,)),
                pltpu.SemaphoreType.DMA((1,)),
                pltpu.SemaphoreType.DMA((n // 2,)),
            ],
            compiler_params=pltpu.CompilerParams(collective_id=0, has_side_effects=True, vmem_limit_bytes=40 * 1024 * 1024),
            name="exchange",
        )(*[pltpu.with_memory_space_constraint(x, pltpu.HBM) for x in operands])
        outs = [((slots, seq_len, rank), bf16), ((slots, rope_dim, seq_len), bf16), ((slots, heads, rank), bf16)]
        c_cache, kr_cache, o_lat = pl.pallas_call(
            functools.partial(finish_kernel, n, (rank + rope_dim) ** -0.5),
            out_shape=[jax.ShapeDtypeStruct(*out) for out in outs],
            in_specs=[vmem] * len(passed),
            out_specs=[hbm] * 3,
            scratch_shapes=[
                pltpu.VMEM((slots, heads, 1), f32),
                pltpu.VMEM((slots, heads, 1), f32),
                pltpu.VMEM((slots, heads, rank), bf16),
                pltpu.SemaphoreType.DMA((3,)),
            ],
            compiler_params=pltpu.CompilerParams(vmem_limit_bytes=8 * 1024 * 1024),
            name="finish",
        )(*got)
        return c_cache, jnp.transpose(kr_cache, (0, 2, 1)), o_lat

    return jax.shard_map(local_step, mesh=mesh, in_specs=(seq_spec, seq_spec, P(None), P("x", None), P("x", None), P("dp"), req_spec, req_spec), out_specs=(req_spec, req_spec, req_spec), check_vma=False)
```

```python
import functools

import jax
import jax.numpy as jnp
from jax import lax
from jax.experimental import pallas as pl
from jax.experimental.pallas import tpu as pltpu
from jax.sharding import PartitionSpec as P

NORM_EPS = 1e-6
MASKED = -3.0e38
MESH = pl.DeviceIdType.MESH
DISTANCES = (3, 2, 1)
RAW = 2


def message_order(chips, slots):
    order = []
    for dist in DISTANCES:
        for core in (0, 1):
            for sign in (-1, 1):
                order.append((sign * dist, core, 0, slots))
    order.insert(4, (0, 1, 0, slots))
    for core in (0, 1):
        order.append((chips // 2, core, 0, slots))
    return order


def normed_rows(rows, gain, first_pos, length):
    rows = rows.astype(jnp.float32)
    inv_rms = lax.rsqrt(jnp.mean(rows * rows, axis=-1, keepdims=True) + NORM_EPS)
    valid = first_pos + lax.broadcasted_iota(jnp.int32, (rows.shape[0], 1), 0) < length
    return jnp.where(valid, rows * inv_rms * gain, 0.0).astype(jnp.bfloat16)


def attend_chunk(r, chip, q_lat, rope_q, recv, kr_out, acc, top, total, own_lens, attn_scale):
    width = own_lens.shape[-1]
    start = pl.multiple_of(chip * width, width)
    rows = recv[r, pl.ds(start, width), :]
    keys = kr_out[r, :, pl.ds(start, width)]
    scores = lax.dot_general(q_lat[r], rows, (((1,), (1,)), ((), ())), preferred_element_type=jnp.float32)
    scores += jnp.dot(rope_q[r], keys, preferred_element_type=jnp.float32)
    pos = start + lax.broadcasted_iota(jnp.int32, (1, width), 1)
    valid = pos < own_lens[r]
    scores = jnp.where(valid, scores * attn_scale, MASKED)
    old_top = top[r]
    new_top = jnp.maximum(old_top, jnp.max(scores, axis=-1, keepdims=True))
    weights = jnp.where(valid, jnp.exp(scores - new_top), 0.0)
    decay = jnp.exp(old_top - new_top)
    top[r] = new_top
    new_total = total[r] * decay + jnp.sum(weights, axis=-1, keepdims=True)
    total[r] = new_total
    mixed = acc[r] * decay + jnp.dot(weights.astype(jnp.bfloat16), rows, preferred_element_type=jnp.float32)
    return mixed, new_total


def exchange_kernel(n, lens_hbm, lens_row_hbm, gain_hbm, cos_hbm, sin_hbm, c_hbm, k_hbm, ql_hbm, qr_hbm, recv, kr_out, acc, top, total, q_lat, rope_q, own_lens, lens, lens_row, gain_ref, cos_ref, sin_ref, send, k_raw, rot, turned, kr_send, kr_recv, q_rope, small_sem, load_sem, send_sem, recv_sem, kr_send_sem, kr_recv_sem):
    me = lax.axis_index("x")
    chips = n // 2
    my_chip, my_core = me // 2, lax.rem(me, 2)
    _, slots, seq_local, rank = send.shape
    half = cos_ref.shape[0]
    attn_scale = (rank + 2 * half) ** -0.5
    messages = message_order(chips, slots)

    def device(dist, core):
        return 2 * lax.rem(my_chip + dist + chips, chips) + lax.rem(my_core + core, 2)

    partners = []
    for dist, core, _, _ in messages:
        if (dist, core) not in partners:
            partners.append((dist, core))
    targets = [device(*partner) for partner in partners]

    barrier = pltpu.get_barrier_semaphore()
    for target in targets:
        pl.semaphore_signal(barrier, inc=1, device_id={"x": target}, device_id_type=MESH)

    def load_c(i):
        dest = me if i == n - 1 else targets[i]
        return pltpu.make_async_copy(c_hbm.at[dest], send.at[dest], load_sem.at[0])

    small = [(lens_hbm, lens), (gain_hbm, gain_ref), (lens_row_hbm, lens_row), (cos_hbm, cos_ref), (sin_hbm, sin_ref), (k_hbm, k_raw), (qr_hbm, q_rope), (ql_hbm, q_lat)]
    small = [pltpu.make_async_copy(src, dst, small_sem.at[i]) for i, (src, dst) in enumerate(small)]

    def norm_rows(dest, first, count):
        def one(slot, carry):
            normed = normed_rows(send[dest, slot], gain, me * seq_local, lens[dest * slots + slot])
            if dest is me:
                recv[slot, pl.ds(pl.multiple_of(me * seq_local, seq_local), seq_local), :] = normed
            else:
                send[dest, slot] = normed
            return carry

        lax.fori_loop(first, first + count, one, 0, unroll=2)

    def c_copy(m):
        dist, core, first, count = messages[m]
        target = device(dist, core)
        return pltpu.make_async_remote_copy(
            src_ref=(c_hbm if m < RAW else send).at[target, pl.ds(first, count)],
            dst_ref=recv.at[pl.ds(first, count), pl.ds(pl.multiple_of(me * seq_local, seq_local), seq_local)],
            send_sem=send_sem.at[0],
            recv_sem=recv_sem.at[dist % chips],
            device_id={"x": target},
            device_id_type=MESH,
        )

    def kr_copy(i):
        return pltpu.make_async_remote_copy(
            src_ref=kr_send.at[targets[i]],
            dst_ref=kr_recv.at[me],
            send_sem=kr_send_sem.at[0],
            recv_sem=kr_recv_sem.at[partners[i][0] % chips],
            device_id={"x": targets[i]},
            device_id_type=MESH,
        )

    def wait_for(region, sem):
        pltpu.make_async_copy(region, region, sem).wait()

    def send_rows(m):
        dist, core, first, count = messages[m]
        if m >= RAW:
            i = partners.index((dist, core))
            norm_rows(targets[i], first, count)
            kr_copy(i).start()
        c_copy(m).start()

    for copy in small[:2]:
        copy.start()
    loads = [i for i in range(n) if i == n - 1 or any(partners[i] == message[:2] for message in messages[RAW:])]
    for i in loads[:3]:
        load_c(i).start()
    for copy in small[2:]:
        copy.start()
    for i in loads[3:]:
        load_c(i).start()

    pl.semaphore_wait(barrier, n - 1)
    for m in range(RAW):
        send_rows(m)
    for copy in small:
        copy.wait()
    lens_vec = lens_row[...]
    for pos in range(seq_local):
        lo = k_raw[pos, :half, :].astype(jnp.float32)
        hi = k_raw[pos, half:, :].astype(jnp.float32)
        cos = cos_ref[:, pos : pos + 1]
        sin = sin_ref[:, pos : pos + 1]
        valid = me * seq_local + pos < lens_vec
        rot[2 * half * pos : 2 * half * pos + half, :] = jnp.where(valid, lo * cos - hi * sin, 0.0)
        rot[2 * half * pos + half : 2 * half * (pos + 1), :] = jnp.where(valid, hi * cos + lo * sin, 0.0)
    requests = n * slots
    for dim in range(half):
        lo = rot[pl.ds(dim, seq_local, stride=2 * half), :]
        hi = rot[pl.ds(half + dim, seq_local, stride=2 * half), :]
        turned[pl.ds(dim, requests, stride=half), :] = jnp.concatenate([lo, hi], axis=0).T
    for dest in range(n):
        kr_send[dest] = turned[dest * slots * half : (dest + 1) * slots * half, :].astype(jnp.bfloat16)
    kr_recv[me] = kr_send[me]

    for i in range(RAW):
        kr_copy(i).start()
    gain = gain_ref[...].astype(jnp.float32).reshape(1, rank)
    wait_for(send.at[pl.ds(0, len(loads))], load_sem.at[0])
    for m in range(RAW, len(messages)):
        send_rows(m)
    norm_rows(me, 0, slots)

    for slot in range(slots):
        rope_q[slot] = q_rope[slot].astype(jnp.float32).T.astype(jnp.bfloat16)
        own_lens[slot] = jnp.full(own_lens.shape[1:], lens[me * slots + slot], jnp.int32)
    acc[...] = jnp.zeros_like(acc)
    top[...] = jnp.full_like(top, MASKED)
    total[...] = jnp.zeros_like(total)

    low_lanes = lax.broadcasted_iota(jnp.int32, (half, 2 * seq_local), 1) < seq_local

    def gather_chip(dist):
        chip = lax.rem(my_chip + dist + chips, chips)
        partner = device(0, 1)
        wait_for(kr_recv.at[pl.ds(2 * chip, 2)] if dist else kr_recv.at[partner], kr_recv_sem.at[-dist % chips])
        start = pl.multiple_of(chip * 2 * seq_local, 2 * seq_local)
        for slot in range(slots):
            even = kr_recv[2 * chip, slot * half : (slot + 1) * half, :].astype(jnp.float32)
            odd = kr_recv[2 * chip + 1, slot * half : (slot + 1) * half, :].astype(jnp.float32)
            kr_out[slot, :half, pl.ds(start, 2 * seq_local)] = jnp.where(low_lanes, even, pltpu.roll(odd, seq_local, 1)).astype(jnp.bfloat16)
            kr_out[slot, half:, pl.ds(start, 2 * seq_local)] = jnp.where(low_lanes, pltpu.roll(even, seq_local, 1), odd).astype(jnp.bfloat16)
        wait_for(recv.at[:, pl.ds(start, 2 * seq_local)] if dist else recv.at[:, pl.ds(pl.multiple_of(partner * seq_local, seq_local), seq_local)], recv_sem.at[-dist % chips])
        for m, (far, _, _, _) in enumerate(messages):
            if (far + dist) % chips == 0:
                if m < RAW:
                    first_pos = pl.multiple_of((2 * chip + lax.rem(my_core + messages[m][1], 2)) * seq_local, seq_local)

                    def one(slot, carry, first_pos=first_pos):
                        recv[slot, pl.ds(first_pos, seq_local), :] = normed_rows(recv[slot, pl.ds(first_pos, seq_local), :], gain, first_pos, lens[me * slots + slot])
                        return carry

                    lax.fori_loop(messages[m][2], sum(messages[m][2:]), one, 0, unroll=2)
        return chip

    for dist in [0] + [sign * far for far in DISTANCES for sign in (1, -1)]:
        chip = gather_chip(dist)

        def one_request(r, carry, chip=chip):
            acc[r], _ = attend_chunk(r, chip, q_lat, rope_q, recv, kr_out, acc, top, total, own_lens, attn_scale)
            return carry

        lax.fori_loop(0, slots, one_request, 0, unroll=2)

    gather_chip(chips // 2)
    wait_for(kr_send.at[pl.ds(0, n - 1)], kr_send_sem.at[0])
    wait_for(send.at[pl.ds(0, n - 1)], send_sem.at[0])


def finish_kernel(n, attn_scale, recv, kr_in, acc, top_in, total_in, q_lat, rope_q, own_lens, c_out, kr_out, o_out, top, total, o_ref, sem):
    chips = n // 2
    slots = acc.shape[0]
    for r in range(slots):
        pltpu.make_async_copy(recv.at[r], c_out.at[r], sem.at[0]).start()
    pltpu.make_async_copy(kr_in, kr_out, sem.at[1]).start()
    top[...] = top_in[...]
    total[...] = total_in[...]
    chip = lax.rem(lax.axis_index("x") // 2 + chips // 2, chips)
    for r in range(slots):
        mixed, weight_sum = attend_chunk(r, chip, q_lat, rope_q, recv, kr_in, acc, top, total, own_lens, attn_scale)
        o_ref[r] = (mixed / weight_sum).astype(jnp.bfloat16)
        pltpu.make_async_copy(o_ref.at[r], o_out.at[r], sem.at[2]).start()
    for i, (src, dst) in enumerate([(recv, c_out), (kr_in, kr_out), (o_ref, o_out)]):
        pltpu.make_async_copy(src, dst, sem.at[i]).wait()


def solution(mesh):
    n = mesh.shape["x"]
    seq_spec = P("dp", "x", None)
    req_spec = P(("dp", "x"), None, None)

    def local_step(c_raw, k_raw, norm_gain, rope_cos, rope_sin, seq_lens, q_lat, q_rope):
        requests, seq_local, rank = c_raw.shape
        slots, heads, _ = q_lat.shape
        rope_dim = k_raw.shape[-1]
        half = rope_dim // 2
        seq_len = n * seq_local
        bf16, f32, i32 = jnp.bfloat16, jnp.float32, jnp.int32
        hbm = pl.BlockSpec(memory_space=pltpu.HBM)
        vmem = pl.BlockSpec(memory_space=pltpu.VMEM)
        passed = [
            ((slots, seq_len, rank), bf16),
            ((slots, rope_dim, seq_len), bf16),
            ((slots, heads, rank), f32),
            ((slots, heads, 1), f32),
            ((slots, heads, 1), f32),
            ((slots, heads, rank), bf16),
            ((slots, heads, rope_dim), bf16),
            ((slots, 1, 2 * seq_local), i32),
        ]
        operands = (
            seq_lens,
            seq_lens.reshape(1, requests),
            norm_gain,
            rope_cos.T,
            rope_sin.T,
            c_raw.reshape(n, slots, seq_local, rank),
            jnp.transpose(k_raw, (1, 2, 0)),
            q_lat,
            jnp.transpose(q_rope, (0, 2, 1)),
        )
        got = pl.pallas_call(
            functools.partial(exchange_kernel, n),
            out_shape=[pltpu.VMEM(*out) for out in passed],
            in_specs=[hbm] * len(operands),
            out_specs=[vmem] * len(passed),
            scratch_shapes=[
                pltpu.SMEM((requests,), i32),
                pltpu.VMEM((1, requests), i32),
                pltpu.VMEM((rank,), bf16),
                pltpu.VMEM((half, seq_local), f32),
                pltpu.VMEM((half, seq_local), f32),
                pltpu.VMEM((n, slots, seq_local, rank), bf16),
                pltpu.VMEM((seq_local, rope_dim, requests), bf16),
                pltpu.VMEM((seq_local * rope_dim, requests), f32),
                pltpu.VMEM((requests * half, 2 * seq_local), f32),
                pltpu.VMEM((n, slots * half, 2 * seq_local), bf16),
                pltpu.VMEM((n, slots * half, 2 * seq_local), bf16),
                pltpu.VMEM((slots, rope_dim, heads), bf16),
                pltpu.SemaphoreType.DMA((8,)),
                pltpu.SemaphoreType.DMA((1,)),
                pltpu.SemaphoreType.DMA((1,)),
                pltpu.SemaphoreType.DMA((n // 2,)),
                pltpu.SemaphoreType.DMA((1,)),
                pltpu.SemaphoreType.DMA((n // 2,)),
            ],
            compiler_params=pltpu.CompilerParams(collective_id=0, has_side_effects=True, vmem_limit_bytes=40 * 1024 * 1024),
            name="exchange",
        )(*[pltpu.with_memory_space_constraint(x, pltpu.HBM) for x in operands])
        outs = [((slots, seq_len, rank), bf16), ((slots, rope_dim, seq_len), bf16), ((slots, heads, rank), bf16)]
        c_cache, kr_cache, o_lat = pl.pallas_call(
            functools.partial(finish_kernel, n, (rank + rope_dim) ** -0.5),
            out_shape=[jax.ShapeDtypeStruct(*out) for out in outs],
            in_specs=[vmem] * len(passed),
            out_specs=[hbm] * 3,
            scratch_shapes=[
                pltpu.VMEM((slots, heads, 1), f32),
                pltpu.VMEM((slots, heads, 1), f32),
                pltpu.VMEM((slots, heads, rank), bf16),
                pltpu.SemaphoreType.DMA((3,)),
            ],
            compiler_params=pltpu.CompilerParams(vmem_limit_bytes=8 * 1024 * 1024),
            name="finish",
        )(*got)
        return c_cache, jnp.transpose(kr_cache, (0, 2, 1)), o_lat

    return jax.shard_map(local_step, mesh=mesh, in_specs=(seq_spec, seq_spec, P(None), P("x", None), P("x", None), P("dp"), req_spec, req_spec), out_specs=(req_spec, req_spec, req_spec), check_vma=False)
```
